128 devices in a mesh: group: 4 (over y), member: 32 (over x, z, core).
Axes of the slice: x: 4, y: 4, z: 4, core: 2. Of those that a mesh axis runs over, the one named last changes fastest.
Arguments:
- samples: bfloat16 [65536, 768], P(('group', 'member')), may hold values from -6 to 6
- cell_of_row: int32 [65536, 1], P(('group', 'member')), may hold values from 0 to 511; in each aligned block of 512 rows (0 to 511, 512 to 1023, ...) at most 2 rows name the same one
- fine_centroids: bfloat16 [131072, 768], P(('group', 'member')), may hold values from -6 to 6
- sharpness: float32 [512], P(('group', 'member')), may hold values from 0.5 to 4
- mid_of_fine: int32 [131072], P(('group', 'member')), may hold values from 0 to 8191, as said below
- mid_centroids: float32 [8192, 768], P(('group', 'member')), may hold values from -6 to 6
- coarse_of_mid: int32 [8192], P(('group', 'member')), may hold values from 0 to 63
- coarse_centroids: float32 [64, 768], replicated, may hold values from -6 to 6
Outputs:
- fine_new: float32 [131072, 768], P(('group', 'member'))
- mids_new: float32 [8192, 768], P(('group', 'member'))
- coarse_new: float32 [64, 768], replicated
- reconstruction: bfloat16 [65536, 768], P(('group', 'member'))
The draws below stay inside these ranges and needn't reach their ends.
Inputs may be any that keep to these rules, and one draw needn't show every extreme that they name: `cell_of_row`: among the rows of one device, no cell is named by more than 2 rows. `mid_of_fine`: fine centroid k's mid centroid lies in [g * 2048, (g + 1) * 2048) with g = k * 4 / 131072 rounded down.
All inputs are finite; a program needn't handle non-finite values.
Results may differ from the reference program's by a relative error of at most 0.007.
Values may be sent and summed in bfloat16 or wider, within the bound.
A program may use at most 64 MiB of HBM per device.

```python
import math
import jax
import jax.numpy as jnp
import numpy as np
from jax import lax

D = 768
FINE = 256
ROWS_DEV = 512
COARSE = 64
ROWS = 65536
CELLS = 512
MIDS = 8192
MOST = 2
N_GROUP = 4
DEVICES = 128


def draw_mid_of_fine(key, part):
    per_group = MIDS // N_GROUP
    group_of_fine = jnp.arange(CELLS * FINE, dtype=jnp.int32) // (CELLS * FINE // N_GROUP)
    offsets = jax.random.randint(jax.random.fold_in(key, 11), (CELLS * FINE,), 0, per_group, dtype=jnp.int32)
    return group_of_fine * per_group + offsets


def set_ends(drawn, key, low, largest):
    longest = drawn.shape.index(max(drawn.shape))
    spots = []
    for shift in (0, 1):
        where = [jax.random.randint(jax.random.fold_in(key, axis), (), 0, length) for axis, length in enumerate(drawn.shape)]
        where[longest] = (where[longest] + shift) % drawn.shape[longest]
        spots.append(tuple(where))
    return drawn.at[spots[0]].set(low).at[spots[1]].set(largest)


def block_levels(stream_key, dims, split, smallest, high):
    def one(axis_at, shards_of):
        heights = jax.random.uniform(jax.random.fold_in(jax.random.fold_in(stream_key, 6), axis_at), (shards_of,), jnp.float32, smallest / len(split), high / len(split))
        return jnp.repeat(jnp.exp(heights), dims[axis_at] // shards_of).reshape((-1,) + (1,) * (len(dims) - axis_at - 1))

    level = one(*split[0])
    for cut in split[1:]:
        level = level * one(*cut)
    return level


def shared_out(key, own, number, rows, amount, top, most, slope):
    order = jax.random.permutation(key, amount)
    crowded, ordinary = portions_of(amount, rows * top, most, slope, True), portions_of(amount, rows * top, most, slope, False)
    places = jnp.arange(amount)

    def named(lengths, turn):
        used = int((lengths > 0).sum())
        fixed = max(1, used // 4)
        passed = fixed + (places - fixed + turn * (used - fixed)) % max(1, amount - fixed)
        return jnp.zeros((amount,), jnp.int32).at[order[jnp.where(places < fixed, places, passed)]].set(jnp.asarray(lengths, jnp.int32))

    lengths = jnp.where(number % 4 == 0, named(crowded, number // 4), named(ordinary, number - number // 4 - 1))
    mixed = jax.random.permutation(jax.random.fold_in(own, 3), amount)
    donor, receiver = mixed[0:amount // 2 * 2:2], mixed[1:amount // 2 * 2:2]
    room = jnp.minimum(lengths[donor] - 1, most - lengths[receiver]) // 2
    room = jnp.where((donor == order[0]) | (receiver == order[0]) | (lengths[receiver] == 0), 0, jnp.maximum(room, 0))
    passed = jax.random.randint(jax.random.fold_in(own, 4), (amount // 2,), 0, 1 << 20) % (room + 1)
    lengths = lengths.at[donor].add(-passed).at[receiver].add(passed)
    members = jnp.searchsorted(jnp.cumsum(lengths), jnp.arange(rows * top), side="right").astype(jnp.int32)
    grid = members.reshape(top, rows).T
    grid = grid[jax.random.permutation(jax.random.fold_in(own, 1), rows)]
    turn = jax.random.randint(jax.random.fold_in(own, 2), (rows, 1), 0, top)
    return jnp.take_along_axis(grid, (jnp.arange(top)[None, :] + turn) % top, axis=1)


def portions_of(number_of, total, reach, lean, full):
    loads = [(1 << 20) // math.isqrt(rank ** lean) + 1 for rank in range(1, number_of + 1)]
    largest = reach if full else min(reach, max(-(-total // number_of), total * loads[0] // sum(loads)))
    least = 1 if total - largest >= number_of - 1 else 0
    counts, surplus = [largest] + [least] * (number_of - 1), total - largest - least * (number_of - 1)
    while surplus > 0:
        free = [i for i in range(1, number_of) if counts[i] < largest] or [i for i in range(1, number_of) if counts[i] < reach]
        mass, remaining = sum([loads[i] for i in free]), surplus
        for i in free:
            extra = min(reach - counts[i], max(1, remaining * loads[i] // mass), surplus)
            counts[i] = counts[i] + extra
            surplus = surplus - extra
    return np.array(counts)


def scatter_about(rng, extent, spread, bound, pieces=(), kind=jnp.bfloat16):
    level = block_levels(rng, extent, pieces, -0.22, 0.18) if pieces else 1.0
    values = jax.random.normal(rng, extent, jnp.float32) * spread * level
    return jnp.minimum(jnp.maximum(values, -bound), bound).astype(kind)


def setup_inputs(seed: int = 0) -> dict:
    key_of = jax.random.split(jax.random.key(seed), 9)
    samples = scatter_about(key_of[0], (ROWS, D), 1.0, 6.0, ((0, 128),))
    cell_of_row_keys = jax.random.split(jax.random.fold_in(key_of[1], 1), ROWS // ROWS_DEV)
    cell_of_row_turns = jax.random.permutation(jax.random.fold_in(key_of[1], 3), ROWS // ROWS_DEV)
    cell_of_row = jax.vmap(lambda own, number: shared_out(jax.random.fold_in(key_of[1], 2), own, number, ROWS_DEV, CELLS, 1, MOST, 2))(cell_of_row_keys, cell_of_row_turns).reshape((ROWS, 1))
    fine_centroids = scatter_about(key_of[2], (CELLS * FINE, D), 1.0, 6.0, ((0, 128),))
    sharpness = jnp.clip(jnp.exp(math.log(4.0) - 2.0794415 * jax.random.uniform(key_of[3], (CELLS,), jnp.float32) ** block_levels(key_of[3], (CELLS,), ((0, 128),), -0.2, 0.2)), 0.5, 4.0)
    mid_of_fine = draw_mid_of_fine(jax.random.fold_in(key_of[8], 71), 0)
    mid_centroids = scatter_about(key_of[5], (MIDS, D), 1.0, 6.0, ((0, 128),), jnp.float32)
    coarse_of_mid = set_ends(jax.random.randint(key_of[6], (MIDS,), 0, COARSE), jax.random.fold_in(key_of[6], 1), 0, COARSE - 1).astype(jnp.int32)
    coarse_centroids = scatter_about(key_of[7], (COARSE, D), 1.0, 6.0, (), jnp.float32)
    return dict(samples=samples, cell_of_row=cell_of_row, fine_centroids=fine_centroids, sharpness=sharpness, mid_of_fine=mid_of_fine, mid_centroids=mid_centroids, coarse_of_mid=coarse_of_mid, coarse_centroids=coarse_centroids)


def reference(samples, cell_of_row, fine_centroids, sharpness, mid_of_fine, mid_centroids, coarse_of_mid, coarse_centroids):
    cell_ids = cell_of_row[:, 0].astype(jnp.int32)
    capacity = MOST * DEVICES
    fine_table = fine_centroids.reshape(CELLS, FINE, D)
    order = jnp.argsort(cell_ids, stable=True).astype(jnp.int32)
    sorted_rows = samples[order]
    padded = jnp.concatenate([sorted_rows, jnp.zeros((capacity, D), samples.dtype)], axis=0)
    cell_counts = jax.ops.segment_sum(jnp.ones_like(cell_ids), cell_ids, CELLS).astype(jnp.int32)
    starts = (jnp.cumsum(cell_counts) - cell_counts).astype(jnp.int32)
    positions = jnp.arange(capacity, dtype=jnp.int32)

    def one_cell(canvas, index):
        start = starts[index]
        block = lax.dynamic_slice_in_dim(padded, start, capacity, 0)
        is_valid = positions < cell_counts[index]
        centres = fine_table[index]
        products = jnp.dot(block, centres.T, preferred_element_type=jnp.float32)
        norms = lax.optimization_barrier(jnp.sum(jnp.square(centres.astype(jnp.float32)), axis=1))
        scores = sharpness[index] * (products - 0.5 * norms[None, :]) / math.sqrt(D)
        highest = lax.optimization_barrier(jnp.max(scores, axis=1, keepdims=True))
        exponent = jnp.exp(scores - highest)
        probs = exponent / lax.optimization_barrier(jnp.sum(exponent, axis=1, keepdims=True))
        resp = jnp.where(is_valid[:, None], probs, 0.0).astype(jnp.bfloat16)
        weighted = jnp.dot(resp.T, block, preferred_element_type=jnp.float32)
        mass_total = lax.optimization_barrier(jnp.sum(resp.astype(jnp.float32), axis=0))
        fine_next = (weighted + centres.astype(jnp.float32)) / (mass_total[:, None] + 1.0)
        rebuilt = jnp.dot(resp, centres, preferred_element_type=jnp.float32).astype(jnp.bfloat16)
        current = lax.dynamic_slice_in_dim(canvas, start, capacity, 0)
        merged = jnp.where(is_valid[:, None], rebuilt, current)
        canvas = lax.dynamic_update_slice_in_dim(canvas, merged, start, 0)
        return (canvas, (fine_next, weighted, mass_total))
    canvas = jnp.zeros((ROWS + capacity, D), jnp.bfloat16)
    canvas, (fine_new, weighted_all, mass_all) = lax.scan(one_cell, canvas, jnp.arange(CELLS, dtype=jnp.int32))
    reconstruction = jnp.zeros((ROWS, D), jnp.bfloat16).at[order].set(canvas[:ROWS])
    mid_sums = jax.ops.segment_sum(weighted_all.reshape(CELLS * FINE, D), mid_of_fine, MIDS)
    mid_counts = jax.ops.segment_sum(mass_all.reshape(CELLS * FINE), mid_of_fine, MIDS)
    mids_new = (mid_sums + mid_centroids) / (mid_counts[:, None] + 1.0)
    coarse_sums = jax.ops.segment_sum(mid_sums, coarse_of_mid, COARSE)
    coarse_counts = jax.ops.segment_sum(mid_counts, coarse_of_mid, COARSE)
    coarse_new = (coarse_sums + coarse_centroids) / (coarse_counts[:, None] + 1.0)
    return (fine_new.reshape(CELLS * FINE, D), mids_new, coarse_new, reconstruction)
```

```python
import functools
import math

import jax
import jax.numpy as jnp
from jax import lax
from jax.experimental import pallas as pl
from jax.experimental.pallas import tpu as pltpu
from jax.sharding import Mesh
from jax.sharding import PartitionSpec as P

MEMBER = ("member_0", "member_1", "member_2")
GROUP_MEMBER = ("group", "member_0", "member_1", "member_2")
RINGS = ("group", "member_0", "member_1")
CORE = "member_2"
EMPTY = 64.0
MESH_ID = pl.DeviceIdType.MESH


def split_up(array, dim, devices):
    dims = array.shape
    pieces = array.reshape(*dims[:dim], devices, dims[dim] // devices, *dims[dim + 1 :])
    return jnp.moveaxis(pieces, dim, 0)


def sent_and_summed(array, axis, dim):
    pieces = split_up(array, dim, lax.axis_size(axis))
    arrived = lax.all_to_all(pieces, axis, split_axis=0, concat_axis=0, tiled=True)
    return arrived.astype(jnp.float32).sum(axis=0)


def sum_in_two_steps(array, axes, dim):
    far, near = axes
    pieces = split_up(array, dim, lax.axis_size(far))
    nearer = sent_and_summed(pieces, near, dim + 1)
    arrived = lax.all_to_all(
        nearer.astype(jnp.bfloat16), far, split_axis=0, concat_axis=0, tiled=True
    )
    return arrived.astype(jnp.float32).sum(axis=0)


def filled_up(lines, devices):
    spare = -len(lines) % devices
    return jnp.pad(lines, [(0, spare)] + [(0, 0)] * (lines.ndim - 1))


def copy_for_each(array, axis):
    copies = jnp.broadcast_to(array, (lax.axis_size(axis), *array.shape))
    return lax.all_to_all(copies, axis, split_axis=0, concat_axis=0, tiled=True)


def in_order(pieces, dim):
    pieces = jnp.moveaxis(pieces, 0, dim)
    dims = pieces.shape
    return pieces.reshape(*dims[:dim], dims[dim] * dims[dim + 1], *dims[dim + 2 :])


def gathered_by_axis(array, axes, dim):
    far, near = axes
    pieces = copy_for_each(copy_for_each(array, far), near)
    return in_order(pieces.swapaxes(0, 1).reshape(-1, *array.shape), dim)


def sum_at_owner(array, axis, dim):
    pieces = split_up(array, dim, lax.axis_size(axis))
    arrived = lax.all_to_all(pieces, axis, split_axis=0, concat_axis=0, tiled=True)
    return arrived.sum(axis=0)


def sum_in_two_steps_2(array, axes, dim):
    far, near = axes
    own = sum_at_owner(split_up(array, dim, lax.axis_size(far)), near, dim + 1)
    return jnp.sum(lax.all_to_all(own, far, 0, 0, tiled=True), axis=0)


def sum_by_parts(array, axes):
    padded = filled_up(array, lax.axis_size(axes[0]) * lax.axis_size(axes[1]))
    whole = gathered_by_axis(sum_in_two_steps_2(padded, axes, 0), axes, 0)
    return lax.slice_in_dim(whole, 0, len(array)).reshape(array.shape)


class Wires:
    def __init__(self, send_sem, recv_sem):
        self.send_sem, self.recv_sem = send_sem, recv_sem
        self.sent, self.arrivals, self.last = 0, 0, []

    def slots(self, number):
        self.arrivals += number
        return self.arrivals - number

    def copy(self, source, target, to, send_at, recv_at):
        return pltpu.make_async_remote_copy(
            src_ref=source,
            dst_ref=target,
            send_sem=self.send_sem.at[send_at],
            recv_sem=self.recv_sem.at[recv_at],
            device_id=to,
            device_id_type=MESH_ID,
        )

    def send(self, source, target, to, recv_at):
        copy = self.copy(source, target, to, self.sent, recv_at)
        self.sent += 1
        copy.start()
        self.last.append(copy)

    def arrived(self, like, to, recv_at):
        self.copy(like, like, to, 0, recv_at).wait_recv()

    def drain(self):
        for copy in self.last:
            copy.wait_send()


def greet(peers):
    barrier = pltpu.get_barrier_semaphore()
    for peer in peers:
        pl.semaphore_signal(barrier, inc=1, device_id=peer, device_id_type=MESH_ID)
    pl.semaphore_wait(barrier, len(peers))


def ring_places(axis):
    me = lax.axis_index(axis)
    return me, lax.rem(me + 1, 4), lax.rem(me + 3, 4), lax.rem(me + 2, 4)


def ring_peers(both_cores):
    core = lax.axis_index(CORE)
    peers = [{CORE: 1 - core}]
    for axis in RINGS:
        for to in ring_places(axis)[1:]:
            peers.append({axis: to})
            if both_cores:
                peers.append({axis: to, CORE: 1 - core})
    return peers


def exchange_kernel(subs, in_ref, out_ref, *scratch):
    stage_a, stage_b, send_sem, recv_sem = scratch
    wires = Wires(send_sem, recv_sem)
    core = lax.axis_index(CORE)
    other = 1 - core
    rings = [ring_places(axis) for axis in RINGS]
    greet(ring_peers(True))
    refs = (in_ref, stage_a, stage_b, out_ref)
    chunks = range(3 * subs)

    def spot(chunk, dim, index, core_at=slice(None)):
        at = [chunk, slice(None), slice(None), slice(None), core_at]
        at[dim + 1] = index
        return tuple(at)

    def start(phase, chunk):
        dim = (chunk + phase) % 3
        source, target = refs[phase], refs[phase + 1]
        axis = RINGS[dim]
        me, up, down, across = rings[dim]
        if phase < 2:
            base = wires.slots(3)
            for way, to in enumerate((across, up, down)):
                wires.send(
                    source.at[spot(chunk, dim, to)],
                    target.at[spot(chunk, dim, me)],
                    {axis: to},
                    base + way,
                )
            own = spot(chunk, dim, me)
        else:
            base = wires.slots(7)
            for way, to in enumerate((across, up, down)):
                for core_at in (0, 1):
                    wires.send(
                        source.at[spot(chunk, dim, to, core_at)],
                        target.at[spot(chunk, dim, me, core)],
                        {axis: to, CORE: core_at},
                        base + 2 * way + core,
                    )
            wires.send(
                source.at[spot(chunk, dim, me, other)],
                target.at[spot(chunk, dim, me, core)],
                {CORE: other},
                base + 6,
            )
            own = spot(chunk, dim, me, core)
        target[own] = source[own]
        return base

    def finish(phase, chunk, base):
        dim = (chunk + phase) % 3
        me, up, _, _ = rings[dim]
        if phase < 2:
            like, number = refs[phase + 1].at[spot(chunk, dim, me)], 3
        else:
            like, number = refs[phase + 1].at[spot(chunk, dim, me, core)], 7
        for at in range(number):
            wires.arrived(like, {RINGS[dim]: up}, base + at)

    running = [start(0, chunk) for chunk in chunks]
    for phase in range(3):
        following = []
        for chunk in chunks:
            finish(phase, chunk, running[chunk])
            if phase < 2:
                following.append(start(phase + 1, chunk))
        running = following
    wires.drain()


def exchanged(array, collective_id):
    chunks, rows, lanes = array.shape
    shape = (chunks, 4, 4, 4, 2, rows // 128, lanes)
    copies = 13 * chunks
    moved = pl.pallas_call(
        functools.partial(exchange_kernel, chunks // 3),
        out_shape=jax.ShapeDtypeStruct(shape, array.dtype),
        in_specs=[pl.BlockSpec(memory_space=pltpu.VMEM)],
        out_specs=pl.BlockSpec(memory_space=pltpu.VMEM),
        scratch_shapes=[
            pltpu.VMEM(shape, array.dtype),
            pltpu.VMEM(shape, array.dtype),
            pltpu.SemaphoreType.DMA((copies,)),
            pltpu.SemaphoreType.DMA((copies,)),
        ],
        compiler_params=pltpu.CompilerParams(
            collective_id=collective_id, has_side_effects=True
        ),
        name=f"exchange_{collective_id}",
    )(array.reshape(shape))
    return moved.reshape(chunks, rows, lanes)


def shards(
    samples,
    cell_of_row,
    fine_centroids,
    sharpness,
    mid_of_fine,
    mid_centroids,
    coarse_of_mid,
    coarse_centroids,
):
    groups = lax.axis_size("group")
    members = lax.axis_size(MEMBER)
    devices = groups * members
    row_count = samples.shape[0]
    feature_width = samples.shape[1]
    cell_dev = sharpness.shape[0]
    fine_count = fine_centroids.shape[0] // cell_dev
    most_rows = 2 * row_count // (cell_dev * devices)
    total_cells = cell_dev * devices
    slots = total_cells * most_rows
    cell_ids = cell_of_row[:, 0]
    place = jnp.arange(row_count, dtype=jnp.int32)
    same = (cell_ids[:, None] == cell_ids[None, :]) & (place[:, None] < place[None, :])
    rank_in_cell = jnp.sum(same.astype(jnp.int32), axis=0)
    slot_index = cell_ids * most_rows + rank_in_cell
    picked = slot_index[None, :] == jnp.arange(slots, dtype=jnp.int32)[:, None]
    used = jnp.any(picked, axis=1)
    picked_rows = picked.astype(jnp.bfloat16)
    lanes = 128
    chunks = feature_width // lanes
    outgoing = jnp.einsum(
        "sr,rcw->csw",
        picked_rows,
        samples.reshape(row_count, chunks, lanes),
        preferred_element_type=jnp.float32,
    )
    outgoing = jnp.where(used[None, :, None], outgoing, EMPTY).astype(jnp.bfloat16)
    arrived = exchanged(outgoing, 0)
    arrived = (
        arrived.reshape(chunks, devices, cell_dev, most_rows, lanes)
        .transpose(2, 1, 3, 0, 4)
        .reshape(cell_dev, devices * most_rows, feature_width)
    )
    fine_local = fine_centroids.reshape(cell_dev, fine_count, feature_width)
    is_valid = arrived[..., 0].astype(jnp.float32) < 0.5 * EMPTY
    products = jnp.einsum("lrd,lkd->lrk", arrived, fine_local, preferred_element_type=jnp.float32)
    fine_float = fine_local.astype(jnp.float32)
    norms = jnp.sum(jnp.square(fine_float), axis=2)
    scores = (
        sharpness[:, None, None] * (products - 0.5 * norms[:, None, :]) / math.sqrt(feature_width)
    )
    highest = jnp.max(scores, axis=2, keepdims=True)
    exponent = jnp.exp(scores - highest)
    probs = exponent / jnp.sum(exponent, axis=2, keepdims=True)
    resp = jnp.where(is_valid[..., None], probs, 0.0).astype(jnp.bfloat16)
    weighted = jnp.einsum("lrk,lrd->lkd", resp, arrived, preferred_element_type=jnp.float32)
    mass_total = jnp.sum(resp.astype(jnp.float32), axis=1)
    fine_new = (weighted + fine_float) / (mass_total[..., None] + 1.0)
    rebuilt = jnp.einsum(
        "lrk,lkd->lrd", resp, fine_local, preferred_element_type=jnp.float32
    ).astype(jnp.bfloat16)
    rebuilt = (
        rebuilt.reshape(cell_dev, devices, most_rows, chunks, lanes)
        .transpose(3, 1, 0, 2, 4)
        .reshape(chunks, slots, lanes)
    )
    returned = exchanged(rebuilt, 1)
    reconstruction = jnp.einsum(
        "sr,csw->rcw", picked_rows, returned, preferred_element_type=jnp.float32
    )
    reconstruction = reconstruction.astype(jnp.bfloat16).reshape(row_count, feature_width)
    group_index = lax.axis_index("group")
    mid_dev = mid_centroids.shape[0]
    mid_group = mid_dev * members
    local_mid = mid_of_fine - group_index * mid_group
    picker = (local_mid[:, None] == jnp.arange(mid_group, dtype=jnp.int32)[None, :]).astype(
        jnp.bfloat16
    )
    weighted_flat = weighted.reshape(cell_dev * fine_count, feature_width)
    mass_flat = mass_total.reshape(cell_dev * fine_count)
    both = jnp.concatenate(
        [
            weighted_flat.astype(jnp.bfloat16),
            jnp.broadcast_to(mass_flat[:, None], (len(mass_flat), 128)).astype(jnp.bfloat16),
        ],
        axis=1,
    )
    mid_part = jnp.dot(picker.T, both, preferred_element_type=jnp.float32)[:, : feature_width + 1]
    own = sum_in_two_steps(mid_part.astype(jnp.bfloat16), (("member_0", "member_1"), "member_2"), 0)
    own_sum, own_count = own[:, :feature_width], own[:, feature_width]
    mids_new = (own_sum + mid_centroids) / (own_count[:, None] + 1.0)
    coarse_total = coarse_centroids.shape[0]
    coarse_route = (
        coarse_of_mid[:, None] == jnp.arange(coarse_total, dtype=jnp.int32)[None, :]
    ).astype(jnp.float32)
    coarse_part = jnp.dot(coarse_route.T, own, precision=lax.Precision.HIGHEST)
    coarse_all = sum_by_parts(coarse_part, (("group", "member_0", "member_1"), "member_2"))
    coarse_sums, coarse_counts = coarse_all[:, :feature_width], coarse_all[:, feature_width]
    coarse_new = (coarse_sums + coarse_centroids) / (coarse_counts[:, None] + 1.0)
    return (
        fine_new.reshape(cell_dev * fine_count, feature_width),
        mids_new,
        coarse_new,
        reconstruction,
    )


def solution(mesh):
    split = Mesh(
        mesh.devices.reshape(mesh.shape["group"], 4, 4, 2),
        ("group", "member_0", "member_1", "member_2"),
    )
    placed = (
        P(GROUP_MEMBER, None),
        P(GROUP_MEMBER, None),
        P(GROUP_MEMBER, None),
        P(GROUP_MEMBER),
        P(GROUP_MEMBER),
        P(GROUP_MEMBER, None),
        P(GROUP_MEMBER),
        P(),
    )
    return jax.shard_map(
        shards,
        mesh=split,
        in_specs=placed,
        out_specs=(P(GROUP_MEMBER, None), P(GROUP_MEMBER, None), P(), P(GROUP_MEMBER, None)),
        check_vma=False,
    )
```

```python
import functools
import math

import jax
import jax.numpy as jnp
from jax import lax
from jax.experimental import pallas as pl
from jax.experimental.pallas import tpu as pltpu
from jax.sharding import Mesh
from jax.sharding import PartitionSpec as P

MEMBER = ("member_0", "member_1", "member_2")
GROUP_MEMBER = ("group", "member_0", "member_1", "member_2")
RINGS = ("group", "member_0", "member_1")
CORE = "member_2"
EMPTY = 64.0
MESH_ID = pl.DeviceIdType.MESH


class Wires:
    def __init__(self, send_sem, recv_sem):
        self.send_sem, self.recv_sem = send_sem, recv_sem
        self.sent, self.arrivals, self.last = 0, 0, []

    def slots(self, number):
        self.arrivals += number
        return self.arrivals - number

    def copy(self, source, target, to, send_at, recv_at):
        return pltpu.make_async_remote_copy(
            src_ref=source,
            dst_ref=target,
            send_sem=self.send_sem.at[send_at],
            recv_sem=self.recv_sem.at[recv_at],
            device_id=to,
            device_id_type=MESH_ID,
        )

    def send(self, source, target, to, recv_at):
        copy = self.copy(source, target, to, self.sent, recv_at)
        self.sent += 1
        copy.start()
        self.last.append(copy)

    def arrived(self, like, to, recv_at):
        self.copy(like, like, to, 0, recv_at).wait_recv()

    def drain(self):
        for copy in self.last:
            copy.wait_send()


def greet(peers):
    barrier = pltpu.get_barrier_semaphore()
    for peer in peers:
        pl.semaphore_signal(barrier, inc=1, device_id=peer, device_id_type=MESH_ID)
    pl.semaphore_wait(barrier, len(peers))


def ring_places(axis):
    me = lax.axis_index(axis)
    return me, lax.rem(me + 1, 4), lax.rem(me + 3, 4), lax.rem(me + 2, 4)


def ring_peers(both_cores):
    core = lax.axis_index(CORE)
    peers = [{CORE: 1 - core}]
    for axis in RINGS:
        for to in ring_places(axis)[1:]:
            peers.append({axis: to})
            if both_cores:
                peers.append({axis: to, CORE: 1 - core})
    return peers


class Exchange:
    def __init__(self, wires, refs):
        self.wires, self.refs = wires, refs
        self.core = lax.axis_index(CORE)
        self.rings = [ring_places(axis) for axis in RINGS]
        self.chunks = range(refs[0].shape[0])
        self.running = [None] * len(self.chunks)

    def spot(self, chunk, dim, index, core_at=slice(None)):
        at = [chunk, slice(None), slice(None), slice(None), core_at]
        at[dim + 1] = index
        return tuple(at)

    def start(self, phase, chunk):
        wires, core, other = self.wires, self.core, 1 - self.core
        dim = (chunk + phase) % 3
        source, target = self.refs[phase], self.refs[phase + 1]
        axis = RINGS[dim]
        me, up, down, across = self.rings[dim]
        if phase < 2:
            base = wires.slots(3)
            for way, to in enumerate((across, up, down)):
                wires.send(
                    source.at[self.spot(chunk, dim, to)],
                    target.at[self.spot(chunk, dim, me)],
                    {axis: to},
                    base + way,
                )
            own = self.spot(chunk, dim, me)
        else:
            base = wires.slots(7)
            for way, to in enumerate((across, up, down)):
                for core_at in (0, 1):
                    wires.send(
                        source.at[self.spot(chunk, dim, to, core_at)],
                        target.at[self.spot(chunk, dim, me, core)],
                        {axis: to, CORE: core_at},
                        base + 2 * way + core,
                    )
            wires.send(
                source.at[self.spot(chunk, dim, me, other)],
                target.at[self.spot(chunk, dim, me, core)],
                {CORE: other},
                base + 6,
            )
            own = self.spot(chunk, dim, me, core)
        target[own] = source[own]
        self.running[chunk] = base

    def finish(self, phase, chunk):
        dim = (chunk + phase) % 3
        me, up, _, _ = self.rings[dim]
        if phase < 2:
            like, number = self.refs[phase + 1].at[self.spot(chunk, dim, me)], 3
        else:
            like, number = self.refs[phase + 1].at[self.spot(chunk, dim, me, self.core)], 7
        for at in range(number):
            self.wires.arrived(like, {RINGS[dim]: up}, self.running[chunk] + at)

    def begin(self):
        for chunk in self.chunks:
            self.start(0, chunk)

    def advance(self, phase):
        for chunk in self.chunks:
            self.finish(phase, chunk)
            if phase < 2:
                self.start(phase + 1, chunk)


class Octet:
    def __init__(self, wires):
        self.wires = wires
        self.me = lax.axis_index("member_0") * 2 + lax.axis_index(CORE)

    def start(self, source_of, target):
        self.base = self.wires.slots(7)
        for step in range(1, 8):
            to = lax.rem(self.me + step, 8)
            where = {"member_0": to // 2, CORE: lax.rem(to, 2)}
            self.wires.send(source_of(to), target, where, self.base + step - 1)

    def finish(self, like):
        for step in range(7):
            self.wires.arrived(like, {CORE: 1 - lax.axis_index(CORE)}, self.base + step)


class Ring:
    def __init__(self, wires, axis):
        self.wires, self.axis = wires, axis
        self.me, self.up, self.down, self.across = ring_places(axis)

    def order(self):
        return (self.across, self.up, self.down)

    def open(self):
        self.base = self.wires.slots(3)

    def send(self, way, source, target):
        self.wires.send(source, target, {self.axis: self.order()[way]}, self.base + way)

    def start(self, source_of, target):
        self.open()
        for way, to in enumerate(self.order()):
            self.send(way, source_of(to), target)

    def finish(self, like):
        for way in range(3):
            self.wires.arrived(like, {self.axis: self.up}, self.base + way)


def rows_kernel(in_ref, map_ref, out_ref, maps_ref, stage_a, stage_b, send_sem, recv_sem):
    wires = Wires(send_sem, recv_sem)
    greet(ring_peers(True))
    moving = Exchange(wires, (in_ref, stage_a, stage_b, out_ref))
    moving.begin()
    octet, ring = Octet(wires), Ring(wires, "member_1")
    mine = maps_ref.at[ring.me, octet.me]
    octet.start(lambda to: map_ref, mine)
    maps_ref[ring.me, octet.me] = map_ref[...]
    octet.finish(mine)
    ring.start(lambda to: maps_ref.at[ring.me], maps_ref.at[ring.me])
    moving.advance(0)
    ring.finish(maps_ref.at[ring.me])
    moving.advance(1)
    moving.advance(2)
    wires.drain()


def rows_sent(array, route):
    chunks, rows, lanes = array.shape
    shape = (chunks, 4, 4, 4, 2, rows // 128, lanes)
    copies = 13 * chunks + 10
    moved, maps = pl.pallas_call(
        rows_kernel,
        out_shape=(
            jax.ShapeDtypeStruct(shape, array.dtype),
            jax.ShapeDtypeStruct((4, 8) + route.shape, route.dtype),
        ),
        in_specs=[pl.BlockSpec(memory_space=pltpu.VMEM)] * 2,
        out_specs=(pl.BlockSpec(memory_space=pltpu.VMEM),) * 2,
        scratch_shapes=[
            pltpu.VMEM(shape, array.dtype),
            pltpu.VMEM(shape, array.dtype),
            pltpu.SemaphoreType.DMA((copies,)),
            pltpu.SemaphoreType.DMA((copies,)),
        ],
        compiler_params=pltpu.CompilerParams(collective_id=0, has_side_effects=True),
        name="rows_sent",
    )(array.reshape(shape), route)
    return moved.reshape(chunks, rows, lanes), maps


def cells_kernel(
    rows_ref,
    fine_ref,
    sharp_ref,
    mid_ref,
    map_ref,
    rebuilt_ref,
    fine_new_ref,
    mid_a_ref,
    mid_b_ref,
    coarse_ref,
    wide,
    back,
    sums,
):
    chunks, rows, lanes = rows_ref.shape
    cells = sharp_ref.shape[0]
    fine = fine_ref.shape[0] // cells
    width = fine_ref.shape[1]
    per_source = 2 * cells
    sources = rows // per_source
    for chunk in range(chunks):
        piece = rows_ref[chunk].astype(jnp.float32)
        wide[chunk] = jnp.where(piece > 0.5 * EMPTY, 0.0, piece)
        if chunk == 0:
            wide[chunks] = jnp.where(piece > 0.5 * EMPTY, 0.0, 1.0)
    for cell in range(cells):
        here = pl.ds(cell * fine, fine)
        centres = fine_ref[here, :]
        centres_wide = centres.astype(jnp.float32)
        norms = jnp.sum(centres_wide * centres_wide, axis=1, keepdims=True)
        lines = [pl.ds(cell * 2 + most, sources, stride=per_source) for most in range(2)]
        block = jnp.concatenate(
            [
                jnp.concatenate([wide[chunk, at, :] for at in lines], axis=0).astype(jnp.bfloat16)
                for chunk in range(chunks + 1)
            ],
            axis=1,
        )
        products = lax.dot_general(
            centres,
            block[:, :width],
            (((1,), (1,)), ((), ())),
            preferred_element_type=jnp.float32,
        )
        scores = (products - 0.5 * norms) * (sharp_ref[cell] / math.sqrt(width))
        exponent = jnp.exp(scores - jnp.max(scores, axis=0, keepdims=True))
        resp = (exponent / jnp.sum(exponent, axis=0, keepdims=True)).astype(jnp.bfloat16)
        weighted = jnp.dot(resp, block, preferred_element_type=jnp.float32)
        share = 1.0 / (weighted[:, width:] + 1.0)
        for chunk in range(chunks):
            at = slice(chunk * lanes, (chunk + 1) * lanes)
            fine_new_ref[here, pl.ds(chunk * lanes, lanes)] = (
                weighted[:, at] + centres_wide[:, at]
            ) * share
        sums[here, :] = weighted.astype(jnp.bfloat16)
        rebuilt = lax.dot_general(
            resp, centres, (((0,), (0,)), ((), ())), preferred_element_type=jnp.float32
        )
        for chunk in range(chunks):
            for most in range(2):
                back[chunk, lines[most], :] = rebuilt[
                    most * sources : (most + 1) * sources, chunk * lanes : (chunk + 1) * lanes
                ]
    for chunk in range(chunks):
        rebuilt_ref[chunk] = back[chunk].astype(jnp.bfloat16)
    step = 256
    split = mid_a_ref.shape[1]
    coarse_ref[...] = jnp.zeros_like(coarse_ref)
    for first in range(0, mid_a_ref.shape[0], step):
        place = lax.broadcasted_iota(jnp.int32, (step, rows), 0) + first
        picker = jnp.where(place == mid_ref[...], 1.0, 0.0).astype(jnp.bfloat16)
        part = jnp.dot(picker, sums[...], preferred_element_type=jnp.float32).astype(jnp.bfloat16)
        mid_a_ref[pl.ds(first, step), :] = part[:, :split]
        mid_b_ref[pl.ds(first, step), :] = part[:, split:]
        level = lax.broadcasted_iota(jnp.int32, (coarse_ref.shape[0], step), 0)
        route = jnp.where(level == map_ref[:, pl.ds(first, step)], 1.0, 0.0).astype(jnp.bfloat16)
        coarse_ref[...] += jnp.dot(route, part, preferred_element_type=jnp.float32)


def cells_done(rows, fine, sharpness, local_mid, mid_map, coarse_total, split):
    chunks, slots, lanes = rows.shape
    width = fine.shape[1]
    wide = width + lanes
    mids = mid_map.shape[1]
    vmem = pl.BlockSpec(memory_space=pltpu.VMEM)
    return pl.pallas_call(
        cells_kernel,
        out_shape=(
            jax.ShapeDtypeStruct((chunks, slots, lanes), jnp.bfloat16),
            jax.ShapeDtypeStruct((len(fine), width), jnp.float32),
            jax.ShapeDtypeStruct((mids, split), jnp.bfloat16),
            jax.ShapeDtypeStruct((mids, wide - split), jnp.bfloat16),
            jax.ShapeDtypeStruct((coarse_total, wide), jnp.float32),
        ),
        in_specs=[vmem, vmem, pl.BlockSpec(memory_space=pltpu.SMEM), vmem, vmem],
        out_specs=(vmem,) * 5,
        scratch_shapes=[
            pltpu.VMEM((chunks + 1, slots, lanes), jnp.float32),
            pltpu.VMEM((chunks, slots, lanes), jnp.float32),
            pltpu.VMEM((len(fine), wide), jnp.bfloat16),
        ],
        compiler_params=pltpu.CompilerParams(vmem_limit_bytes=48 * 1024 * 1024),
        name="cells_done",
    )(rows, fine, sharpness, local_mid, mid_map)


def sums_kernel(
    rows_ref,
    mid_a_ref,
    mid_b_ref,
    coarse_ref,
    out_ref,
    own_ref,
    total_ref,
    stage_a,
    stage_b,
    half_a,
    half_b,
    core_a,
    core_b,
    near_a,
    near_b,
    line_a,
    line_b,
    far_a,
    far_b,
    first_sum,
    second_sum,
    third_sum,
    send_sem,
    recv_sem,
):
    wires = Wires(send_sem, recv_sem)
    core = lax.axis_index(CORE)
    other = 1 - core
    greet(ring_peers(True))
    split = mid_a_ref.shape[-1]
    xs, zs, ys = Ring(wires, "member_0"), Ring(wires, "member_1"), Ring(wires, "group")
    xs_late, zs_late = Ring(wires, "member_0"), Ring(wires, "member_1")
    octet = Octet(wires)

    order_a = xs.order() + (xs.me,)
    order_b = zs.order() + (zs.me,)
    swap = wires.slots(8)
    for way in range(4):
        wires.send(
            mid_a_ref.at[order_a[way], :, other], core_a.at[order_a[way]], {CORE: other}, swap + way
        )
        wires.send(
            mid_b_ref.at[:, order_b[way], other],
            core_b.at[:, order_b[way]],
            {CORE: other},
            swap + 4 + way,
        )
    octet.start(lambda to: coarse_ref.at[to], first_sum.at[octet.me])
    first_sum[octet.me] = coarse_ref[octet.me]
    moving = Exchange(wires, (rows_ref, stage_a, stage_b, out_ref))
    moving.begin()

    xs.open()
    zs.open()
    for way in range(4):
        to = order_a[way]
        wires.arrived(core_a.at[to], {CORE: other}, swap + way)
        for z in range(4):
            half_a[to, z] = (
                mid_a_ref[to, z, core].astype(jnp.float32) + core_a[to, z].astype(jnp.float32)
            ).astype(jnp.bfloat16)
        if way < 3:
            xs.send(way, half_a.at[to], near_a.at[xs.me])
        to = order_b[way]
        wires.arrived(core_b.at[:, to], {CORE: other}, swap + 4 + way)
        for x in range(4):
            half_b[x, to] = (
                mid_b_ref[x, to, core].astype(jnp.float32) + core_b[x, to].astype(jnp.float32)
            ).astype(jnp.bfloat16)
        if way < 3:
            zs.send(way, half_b.at[:, to], near_b.at[zs.me])

    octet.finish(first_sum.at[octet.me])
    second_sum[zs.me] = sum(first_sum[at] for at in range(8))
    zs_coarse = Ring(wires, "member_1")
    zs_coarse.start(lambda to: second_sum.at[zs.me], second_sum.at[zs.me])

    moving.advance(0)

    zs_coarse.finish(second_sum.at[zs.me])
    third_sum[ys.me] = sum(second_sum[at] for at in range(4))
    ys.start(lambda to: third_sum.at[ys.me], third_sum.at[ys.me])

    xs.finish(near_a.at[xs.me])
    for z in range(4):
        line_a[z] = (
            half_a[xs.me, z].astype(jnp.float32)
            + sum(near_a[at, z].astype(jnp.float32) for at in xs.order())
        ).astype(jnp.bfloat16)
    zs_late.start(lambda to: line_a.at[to], far_a.at[zs.me])
    zs.finish(near_b.at[zs.me])
    for x in range(4):
        line_b[x] = (
            half_b[x, zs.me].astype(jnp.float32)
            + sum(near_b[at, x].astype(jnp.float32) for at in zs.order())
        ).astype(jnp.bfloat16)
    xs_late.start(lambda to: line_b.at[to], far_b.at[xs.me])

    moving.advance(1)

    ys.finish(third_sum.at[ys.me])
    total_ref[octet.me] = sum(third_sum[at] for at in range(4))
    octet.start(lambda to: total_ref.at[octet.me], total_ref.at[octet.me])

    zs_late.finish(far_a.at[zs.me])
    own_ref[:, pl.ds(0, split)] = line_a[zs.me].astype(jnp.float32) + sum(
        far_a[at].astype(jnp.float32) for at in zs.order()
    )
    xs_late.finish(far_b.at[xs.me])
    own_ref[:, pl.ds(split, mid_b_ref.shape[-1])] = line_b[xs.me].astype(jnp.float32) + sum(
        far_b[at].astype(jnp.float32) for at in xs.order()
    )
    moving.advance(2)
    octet.finish(total_ref.at[octet.me])
    wires.drain()


def sums_sent(array, mid_a, mid_b, coarse):
    chunks, rows, lanes = array.shape
    shape = (chunks, 4, 4, 4, 2, rows // 128, lanes)
    mid_dev = len(mid_a) // 32
    wide_a, wide_b = mid_a.shape[1], mid_b.shape[1]
    eighth = (len(coarse) // 8, coarse.shape[1])
    copies = 13 * chunks + 8 + 7 + 3 + 3 + 3 + 3 + 3 + 3 + 7
    vmem = pl.BlockSpec(memory_space=pltpu.VMEM)
    moved, own, total = pl.pallas_call(
        sums_kernel,
        out_shape=(
            jax.ShapeDtypeStruct(shape, array.dtype),
            jax.ShapeDtypeStruct((mid_dev, wide_a + wide_b), jnp.float32),
            jax.ShapeDtypeStruct((8,) + eighth, jnp.float32),
        ),
        in_specs=[vmem] * 4,
        out_specs=(vmem,) * 3,
        scratch_shapes=[
            pltpu.VMEM(shape, array.dtype),
            pltpu.VMEM(shape, array.dtype),
            pltpu.VMEM((4, 4, mid_dev, wide_a), jnp.bfloat16),
            pltpu.VMEM((4, 4, mid_dev, wide_b), jnp.bfloat16),
            pltpu.VMEM((4, 4, mid_dev, wide_a), jnp.bfloat16),
            pltpu.VMEM((4, 4, mid_dev, wide_b), jnp.bfloat16),
            pltpu.VMEM((4, 4, mid_dev, wide_a), jnp.bfloat16),
            pltpu.VMEM((4, 4, mid_dev, wide_b), jnp.bfloat16),
            pltpu.VMEM((4, mid_dev, wide_a), jnp.bfloat16),
            pltpu.VMEM((4, mid_dev, wide_b), jnp.bfloat16),
            pltpu.VMEM((4, mid_dev, wide_a), jnp.bfloat16),
            pltpu.VMEM((4, mid_dev, wide_b), jnp.bfloat16),
            pltpu.VMEM((8,) + eighth, jnp.float32),
            pltpu.VMEM((4,) + eighth, jnp.float32),
            pltpu.VMEM((4,) + eighth, jnp.float32),
            pltpu.SemaphoreType.DMA((copies,)),
            pltpu.SemaphoreType.DMA((copies,)),
        ],
        compiler_params=pltpu.CompilerParams(
            collective_id=1, has_side_effects=True, vmem_limit_bytes=56 * 1024 * 1024
        ),
        name="sums_sent",
    )(
        array.reshape(shape),
        mid_a.reshape(4, 4, 2, mid_dev, wide_a),
        mid_b.reshape(4, 4, 2, mid_dev, wide_b),
        coarse.reshape((8,) + eighth),
    )
    return moved.reshape(chunks, rows, lanes), own, total.reshape(coarse.shape)


def shards(
    samples,
    cell_of_row,
    fine_centroids,
    sharpness,
    mid_of_fine,
    mid_centroids,
    coarse_of_mid,
    coarse_centroids,
):
    groups = lax.axis_size("group")
    members = lax.axis_size(MEMBER)
    devices = groups * members
    row_count = samples.shape[0]
    feature_width = samples.shape[1]
    cell_dev = sharpness.shape[0]
    most_rows = 2 * row_count // (cell_dev * devices)
    total_cells = cell_dev * devices
    slots = total_cells * most_rows
    cell_ids = cell_of_row[:, 0]
    place = jnp.arange(row_count, dtype=jnp.int32)
    same = (cell_ids[:, None] == cell_ids[None, :]) & (place[:, None] < place[None, :])
    rank_in_cell = jnp.sum(same.astype(jnp.int32), axis=0)
    slot_index = cell_ids * most_rows + rank_in_cell
    picked = slot_index[None, :] == jnp.arange(slots, dtype=jnp.int32)[:, None]
    used = jnp.any(picked, axis=1)
    picked_rows = picked.astype(jnp.bfloat16)
    lanes = 128
    chunks = feature_width // lanes
    outgoing = jnp.einsum(
        "sr,rcw->csw",
        picked_rows,
        samples.reshape(row_count, chunks, lanes),
        preferred_element_type=jnp.float32,
    )
    outgoing = jnp.where(used[None, :, None], outgoing, EMPTY).astype(jnp.bfloat16)
    arrived, maps = rows_sent(outgoing, jnp.pad(coarse_of_mid, (0, lanes - len(coarse_of_mid)))[None])
    mid_dev = mid_centroids.shape[0]
    mid_group = mid_dev * members
    mid_map = maps.reshape(4, 4, 2, lanes)[..., :mid_dev].swapaxes(0, 1).reshape(1, mid_group)
    local_mid = (mid_of_fine - lax.axis_index("group") * mid_group)[None]
    coarse_total = coarse_centroids.shape[0]
    split = 4 * lanes
    rebuilt, fine_new, mid_a, mid_b, coarse_part = cells_done(
        arrived, fine_centroids, sharpness, local_mid, mid_map, coarse_total, split
    )
    returned, own, coarse_all = sums_sent(rebuilt, mid_a, mid_b, coarse_part)
    reconstruction = jnp.einsum(
        "sr,csw->rcw", picked_rows, returned, preferred_element_type=jnp.float32
    )
    reconstruction = reconstruction.astype(jnp.bfloat16).reshape(row_count, feature_width)
    own_sum, own_count = own[:, :feature_width], own[:, feature_width]
    mids_new = (own_sum + mid_centroids) / (own_count[:, None] + 1.0)
    coarse_sums, coarse_counts = coarse_all[:, :feature_width], coarse_all[:, feature_width]
    coarse_new = (coarse_sums + coarse_centroids) / (coarse_counts[:, None] + 1.0)
    return fine_new, mids_new, coarse_new, reconstruction


def solution(mesh):
    split = Mesh(
        mesh.devices.reshape(mesh.shape["group"], 4, 4, 2),
        ("group", "member_0", "member_1", "member_2"),
    )
    placed = (
        P(GROUP_MEMBER, None),
        P(GROUP_MEMBER, None),
        P(GROUP_MEMBER, None),
        P(GROUP_MEMBER),
        P(GROUP_MEMBER),
        P(GROUP_MEMBER, None),
        P(GROUP_MEMBER),
        P(),
    )
    return jax.shard_map(
        shards,
        mesh=split,
        in_specs=placed,
        out_specs=(P(GROUP_MEMBER, None), P(GROUP_MEMBER, None), P(), P(GROUP_MEMBER, None)),
        check_vma=False,
    )
```

```python
import math

import jax
import jax.numpy as jnp
from jax import lax
from jax.experimental import pallas as pl
from jax.experimental.pallas import tpu as pltpu
from jax.sharding import Mesh
from jax.sharding import PartitionSpec as P

MEMBER = ("member_0", "member_1", "member_2")
GROUP_MEMBER = ("group", "member_0", "member_1", "member_2")
RINGS = ("group", "member_0", "member_1")
CORE = "member_2"
EMPTY = 64.0
MESH_ID = pl.DeviceIdType.MESH


class Wires:
    def __init__(self, send_sem, recv_sem):
        self.send_sem, self.recv_sem = send_sem, recv_sem
        self.sent, self.arrivals, self.last = 0, 0, []

    def slots(self, number):
        self.arrivals += number
        return self.arrivals - number

    def copy(self, source, target, to, send_at, recv_at):
        return pltpu.make_async_remote_copy(
            src_ref=source,
            dst_ref=target,
            send_sem=self.send_sem.at[send_at],
            recv_sem=self.recv_sem.at[recv_at],
            device_id=to,
            device_id_type=MESH_ID,
        )

    def send(self, source, target, to, recv_at):
        copy = self.copy(source, target, to, self.sent, recv_at)
        self.sent += 1
        copy.start()
        self.last.append(copy)

    def arrived(self, like, to, recv_at):
        self.copy(like, like, to, 0, recv_at).wait_recv()

    def drain(self):
        for copy in self.last:
            copy.wait_send()


def greet(peers):
    barrier = pltpu.get_barrier_semaphore()
    for peer in peers:
        pl.semaphore_signal(barrier, inc=1, device_id=peer, device_id_type=MESH_ID)
    pl.semaphore_wait(barrier, len(peers))


def ring_places(axis):
    me = lax.axis_index(axis)
    return me, lax.rem(me + 1, 4), lax.rem(me + 3, 4), lax.rem(me + 2, 4)


def ring_peers(both_cores):
    core = lax.axis_index(CORE)
    peers = [{CORE: 1 - core}]
    for axis in RINGS:
        for to in ring_places(axis)[1:]:
            peers.append({axis: to})
            if both_cores:
                peers.append({axis: to, CORE: 1 - core})
    return peers


class Exchange:
    def __init__(self, wires, refs):
        self.wires, self.refs = wires, refs
        self.core = lax.axis_index(CORE)
        self.rings = [ring_places(axis) for axis in RINGS]
        self.chunks = range(refs[0].shape[0])
        self.running = [None] * len(self.chunks)

    def spot(self, chunk, dim, index, core_at=slice(None)):
        at = [chunk, slice(None), slice(None), slice(None), core_at]
        at[dim + 1] = index
        return tuple(at)

    def start(self, phase, chunk):
        wires, core, other = self.wires, self.core, 1 - self.core
        dim = (chunk + phase) % 3
        source, target = self.refs[phase], self.refs[phase + 1]
        axis = RINGS[dim]
        me, up, down, across = self.rings[dim]
        if phase < 2:
            base = wires.slots(3)
            for way, to in enumerate((across, up, down)):
                wires.send(
                    source.at[self.spot(chunk, dim, to)],
                    target.at[self.spot(chunk, dim, me)],
                    {axis: to},
                    base + way,
                )
            own = self.spot(chunk, dim, me)
        else:
            base = wires.slots(7)
            for way, to in enumerate((across, up, down)):
                for core_at in (0, 1):
                    wires.send(
                        source.at[self.spot(chunk, dim, to, core_at)],
                        target.at[self.spot(chunk, dim, me, core)],
                        {axis: to, CORE: core_at},
                        base + 2 * way + core,
                    )
            wires.send(
                source.at[self.spot(chunk, dim, me, other)],
                target.at[self.spot(chunk, dim, me, core)],
                {CORE: other},
                base + 6,
            )
            own = self.spot(chunk, dim, me, core)
        target[own] = source[own]
        self.running[chunk] = base

    def finish(self, phase, chunk):
        dim = (chunk + phase) % 3
        me, up, _, _ = self.rings[dim]
        if phase < 2:
            like, number = self.refs[phase + 1].at[self.spot(chunk, dim, me)], 3
        else:
            like, number = self.refs[phase + 1].at[self.spot(chunk, dim, me, self.core)], 7
        for at in range(number):
            self.wires.arrived(like, {RINGS[dim]: up}, self.running[chunk] + at)

    def begin(self):
        for chunk in self.chunks:
            self.start(0, chunk)

    def advance(self, phase):
        for chunk in self.chunks:
            self.finish(phase, chunk)
            if phase < 2:
                self.start(phase + 1, chunk)


class Octet:
    def __init__(self, wires):
        self.wires = wires
        self.me = lax.axis_index("member_0") * 2 + lax.axis_index(CORE)

    def start(self, source_of, target):
        self.base = self.wires.slots(7)
        for step in range(1, 8):
            to = lax.rem(self.me + step, 8)
            where = {"member_0": to // 2, CORE: lax.rem(to, 2)}
            self.wires.send(source_of(to), target, where, self.base + step - 1)

    def finish(self, like):
        for step in range(7):
            self.wires.arrived(like, {CORE: 1 - lax.axis_index(CORE)}, self.base + step)


class Ring:
    def __init__(self, wires, axis):
        self.wires, self.axis = wires, axis
        self.me, self.up, self.down, self.across = ring_places(axis)

    def order(self):
        return (self.across, self.up, self.down)

    def open(self):
        self.base = self.wires.slots(3)

    def send(self, way, source, target):
        self.wires.send(source, target, {self.axis: self.order()[way]}, self.base + way)

    def start(self, source_of, target):
        self.open()
        for way, to in enumerate(self.order()):
            self.send(way, source_of(to), target)

    def finish(self, like):
        for way in range(3):
            self.wires.arrived(like, {self.axis: self.up}, self.base + way)


def diagonal(rows, lanes):
    return lax.broadcasted_iota(jnp.int32, (rows, lanes), 0) == lax.broadcasted_iota(
        jnp.int32, (rows, lanes), 1
    )


def as_column(row, rows):
    return jnp.sum(
        jnp.where(diagonal(rows, row.shape[1]), row, jnp.zeros_like(row)), axis=1, keepdims=True
    )


def step_kernel(
    samples_ref,
    cell_ref,
    fine_ref,
    sharp_ref,
    mid_ref,
    mids_ref,
    route_ref,
    coarse_ref,
    fine_new_ref,
    mids_new_ref,
    coarse_new_ref,
    rec_ref,
    outgoing,
    there_a,
    there_b,
    arrived,
    rebuilt,
    back_a,
    back_b,
    returned,
    wide,
    back,
    resps,
    sums,
    chosen,
    maps,
    give,
    core_in,
    half_a,
    half_b,
    near_a,
    near_b,
    line_a,
    line_b,
    far_a,
    far_b,
    give_m,
    core_m,
    half_m,
    near_m,
    line_m,
    far_m,
    part_c,
    first_sum,
    second_sum,
    third_sum,
    total,
    send_sem,
    recv_sem,
):
    f32, bf16 = jnp.float32, jnp.bfloat16
    wires = Wires(send_sem, recv_sem)
    core = lax.axis_index(CORE)
    other = 1 - core
    chunks, lanes = outgoing.shape[0], outgoing.shape[-1]
    row_count, width = samples_ref.shape
    slots = chosen.shape[1]
    cells = sharp_ref.shape[0]
    fine = fine_ref.shape[0] // cells
    per_source = 2 * cells
    sources = slots // per_source
    mid_dev = mids_ref.shape[0]
    split = half_a.shape[-1]

    cell_row = cell_ref[...]
    cell_column = as_column(cell_row, row_count)
    earlier = lax.broadcasted_iota(jnp.int32, (row_count, row_count), 0) < lax.broadcasted_iota(
        jnp.int32, (row_count, row_count), 1
    )
    rank = jnp.sum(
        jnp.where((cell_column == cell_row) & earlier, 1, 0), axis=0, keepdims=True
    )
    slot_row = cell_row * 2 + rank
    place = lax.broadcasted_iota(jnp.int32, (slots, row_count), 0)
    picked = jnp.where(place == slot_row, 1.0, 0.0).astype(bf16)
    used = jnp.dot(picked, jnp.ones((row_count, lanes), bf16), preferred_element_type=f32) > 0.5

    greet(ring_peers(True))
    moving = Exchange(wires, (outgoing, there_a, there_b, arrived))
    for chunk in range(chunks):
        lines = jnp.dot(
            picked, samples_ref[:, pl.ds(chunk * lanes, lanes)], preferred_element_type=f32
        )
        lines = jnp.where(used, lines, EMPTY)
        outgoing[chunk] = lines.reshape(outgoing.shape[1:]).astype(bf16)
        moving.start(0, chunk)
    octet = Octet(wires)
    xs, zs, ys = Ring(wires, "member_0"), Ring(wires, "member_1"), Ring(wires, "group")
    maps_ring = Ring(wires, "member_1")
    octet.start(lambda to: route_ref, maps.at[zs.me, octet.me])
    maps[zs.me, octet.me] = route_ref[...]
    slot_column = as_column(slot_row, row_count)
    along = lax.broadcasted_iota(jnp.int32, (row_count, slots), 1)
    chosen[...] = jnp.where(along == slot_column, 1.0, 0.0).astype(bf16)
    octet.finish(maps.at[zs.me, octet.me])
    maps_ring.start(lambda to: maps.at[zs.me], maps.at[zs.me])
    moving.advance(0)
    maps_ring.finish(maps.at[zs.me])
    moving.advance(1)
    moving.advance(2)

    for chunk in range(chunks):
        piece = arrived[chunk].astype(f32).reshape(slots, lanes)
        wide[chunk] = jnp.where(piece > 0.5 * EMPTY, 0.0, piece)
        if chunk == 0:
            wide[chunks] = jnp.where(piece > 0.5 * EMPTY, 0.0, 1.0)

    def cell_rows(cell, number):
        spots = [pl.ds(cell * 2 + most, sources, stride=per_source) for most in range(2)]
        return jnp.concatenate(
            [
                jnp.concatenate([wide[chunk, at, :] for at in spots], axis=0).astype(bf16)
                for chunk in range(number)
            ],
            axis=1,
        )

    for cell in range(cells):
        centres = fine_ref[pl.ds(cell * fine, fine), :]
        centres_wide = centres.astype(f32)
        norms = jnp.sum(centres_wide * centres_wide, axis=1, keepdims=True)
        products = lax.dot_general(
            centres,
            cell_rows(cell, chunks),
            (((1,), (1,)), ((), ())),
            preferred_element_type=f32,
        )
        scores = (products - 0.5 * norms) * (sharp_ref[cell] / math.sqrt(width))
        exponent = jnp.exp(scores - jnp.max(scores, axis=0, keepdims=True))
        resp = (exponent / jnp.sum(exponent, axis=0, keepdims=True)).astype(bf16)
        resps[cell] = resp
        lines = lax.dot_general(resp, centres, (((0,), (0,)), ((), ())), preferred_element_type=f32)
        for chunk in range(chunks):
            for most in range(2):
                back[chunk, pl.ds(cell * 2 + most, sources, stride=per_source), :] = lines[
                    most * sources : (most + 1) * sources, chunk * lanes : (chunk + 1) * lanes
                ]
    homing = Exchange(wires, (rebuilt, back_a, back_b, returned))
    for chunk in range(chunks):
        rebuilt[chunk] = back[chunk].reshape(rebuilt.shape[1:]).astype(bf16)
        homing.start(0, chunk)

    for cell in range(cells):
        here = pl.ds(cell * fine, fine)
        weighted = jnp.dot(resps[cell], cell_rows(cell, chunks + 1), preferred_element_type=f32)
        sums[here, :] = weighted.astype(bf16)
        centres_wide = fine_ref[here, :].astype(f32)
        share = 1.0 / (weighted[:, width:] + 1.0)
        for chunk in range(chunks):
            at = slice(chunk * lanes, (chunk + 1) * lanes)
            fine_new_ref[here, pl.ds(chunk * lanes, lanes)] = (
                weighted[:, at] + centres_wide[:, at]
            ) * share

    rows_of = 4 * mid_dev
    local_mid = mid_ref[...] - lax.axis_index("group") * (32 * mid_dev)
    spread = lax.broadcasted_iota(jnp.int32, (rows_of, fine_ref.shape[0]), 0)
    spread = (spread // mid_dev) * (2 * mid_dev) + spread % mid_dev

    def mid_part(x, core_at):
        wanted = local_mid - (x * 8 + core_at) * mid_dev
        picker = jnp.where(spread == wanted, 1.0, 0.0).astype(bf16)
        return jnp.dot(picker, sums[...], preferred_element_type=f32)

    def mass_row(part, z):
        tile = part[z * mid_dev : (z + 1) * mid_dev, width:]
        return jnp.sum(
            jnp.where(diagonal(mid_dev, lanes), tile, 0.0), axis=0, keepdims=True
        )

    order_x = xs.order() + (xs.me,)
    swap, swap_m = wires.slots(4), wires.slots(4)
    for way, x in enumerate(order_x):
        part = mid_part(x, other)
        for z in range(4):
            give[x, z] = part[z * mid_dev : (z + 1) * mid_dev, :width].astype(bf16)
            give_m[x, z] = mass_row(part, z)
        wires.send(give.at[x], core_in.at[x], {CORE: other}, swap + way)
        wires.send(give_m.at[x], core_m.at[x], {CORE: other}, swap_m + way)
    xs_m = Ring(wires, "member_0")
    xs.open()
    xs_m.open()
    level = lax.broadcasted_iota(jnp.int32, (coarse_ref.shape[0], lanes), 0)
    coarse_part = jnp.zeros((coarse_ref.shape[0], width), f32)
    coarse_mass = jnp.zeros((coarse_ref.shape[0], lanes), f32)
    for way, x in enumerate(order_x):
        part = mid_part(x, core)
        wires.arrived(core_in.at[x], {CORE: other}, swap + way)
        wires.arrived(core_m.at[x], {CORE: other}, swap_m + way)
        for z in range(4):
            half = part[z * mid_dev : (z + 1) * mid_dev, :width] + core_in[x, z].astype(f32)
            half = half.astype(bf16)
            half_a[x, z] = half[:, :split]
            half_b[z, x] = half[:, split:]
            masses = mass_row(part, z) + core_m[x, z]
            half_m[x, z] = masses
            goes = level == maps[z, x * 2 + core]
            coarse_mass += jnp.where(goes, masses, 0.0)
            coarse_part += jnp.dot(
                jnp.where(goes, 1.0, 0.0).astype(bf16)[:, :mid_dev],
                half,
                preferred_element_type=f32,
            )
        if way < 3:
            xs.send(way, half_a.at[x], near_a.at[xs.me])
            xs_m.send(way, half_m.at[x], near_m.at[xs.me])
    zs.start(lambda to: half_b.at[to], near_b.at[zs.me])
    coarse_mass = jnp.broadcast_to(jnp.sum(coarse_mass, axis=1, keepdims=True), coarse_mass.shape)
    for at in range(8):
        part_c[at, :, pl.ds(0, width)] = coarse_part[8 * at : 8 * at + 8]
        part_c[at, :, pl.ds(width, lanes)] = coarse_mass[8 * at : 8 * at + 8]
    octet.start(lambda to: part_c.at[to], first_sum.at[octet.me])
    first_sum[octet.me] = part_c[octet.me]

    homing.advance(0)

    octet.finish(first_sum.at[octet.me])
    second_sum[zs.me] = sum(first_sum[at] for at in range(8))
    zs_coarse = Ring(wires, "member_1")
    zs_coarse.start(lambda to: second_sum.at[zs.me], second_sum.at[zs.me])

    xs.finish(near_a.at[xs.me])
    xs_m.finish(near_m.at[xs.me])
    for z in range(4):
        line_a[z] = (
            half_a[xs.me, z].astype(f32) + sum(near_a[at, z].astype(f32) for at in xs.order())
        ).astype(bf16)
        line_m[z] = half_m[xs.me, z] + sum(near_m[at, z] for at in xs.order())
    zs_late, zs_m, xs_late = Ring(wires, "member_1"), Ring(wires, "member_1"), Ring(wires, "member_0")
    zs_late.start(lambda to: line_a.at[to], far_a.at[zs.me])
    zs_m.start(lambda to: line_m.at[to], far_m.at[zs.me])
    zs.finish(near_b.at[zs.me])
    for x in range(4):
        line_b[x] = (
            half_b[zs.me, x].astype(f32) + sum(near_b[at, x].astype(f32) for at in zs.order())
        ).astype(bf16)
    xs_late.start(lambda to: line_b.at[to], far_b.at[xs.me])

    zs_coarse.finish(second_sum.at[zs.me])
    third_sum[ys.me] = sum(second_sum[at] for at in range(4))
    ys.start(lambda to: third_sum.at[ys.me], third_sum.at[ys.me])

    homing.advance(1)

    ys.finish(third_sum.at[ys.me])
    total[octet.me] = sum(third_sum[at] for at in range(4))
    octet.start(lambda to: total.at[octet.me], total.at[octet.me])

    zs_late.finish(far_a.at[zs.me])
    zs_m.finish(far_m.at[zs.me])
    xs_late.finish(far_b.at[xs.me])
    masses = line_m[zs.me] + sum(far_m[at] for at in zs.order())
    share = 1.0 / (as_column(masses, mid_dev) + 1.0)
    own_a = line_a[zs.me].astype(f32) + sum(far_a[at].astype(f32) for at in zs.order())
    own_b = line_b[xs.me].astype(f32) + sum(far_b[at].astype(f32) for at in xs.order())
    mids_new_ref[:, pl.ds(0, split)] = (own_a + mids_ref[:, pl.ds(0, split)]) * share
    mids_new_ref[:, pl.ds(split, split)] = (own_b + mids_ref[:, pl.ds(split, split)]) * share

    octet.finish(total.at[octet.me])
    for at in range(8):
        here = pl.ds(8 * at, 8)
        share = 1.0 / (total[at, :, pl.ds(width, lanes)] + 1.0)
        for chunk in range(chunks):
            there = pl.ds(chunk * lanes, lanes)
            coarse_new_ref[here, there] = (total[at, :, there] + coarse_ref[here, there]) * share
    for chunk in range(chunks):
        homing.finish(2, chunk)
        lines = returned[chunk].astype(f32).reshape(slots, lanes).astype(bf16)
        rec_ref[:, pl.ds(chunk * lanes, lanes)] = jnp.dot(
            chosen[...], lines, preferred_element_type=f32
        ).astype(bf16)
    wires.drain()


def shards(
    samples,
    cell_of_row,
    fine_centroids,
    sharpness,
    mid_of_fine,
    mid_centroids,
    coarse_of_mid,
    coarse_centroids,
):
    row_count, width = samples.shape
    cells = sharpness.shape[0]
    fine_total = fine_centroids.shape[0]
    fine = fine_total // cells
    mid_dev = mid_centroids.shape[0]
    coarse_total = coarse_centroids.shape[0]
    lanes = 128
    chunks = width // lanes
    slots = 128 * 2 * cells
    split = width // 2
    moved = (chunks, 4, 4, 4, 2, 2 * cells, lanes)
    eighth = (coarse_total // 8, width + lanes)
    copies = 2 * 13 * chunks + 3 * 7 + 9 * 3 + 8
    f32, bf16 = jnp.float32, jnp.bfloat16
    vmem = pl.BlockSpec(memory_space=pltpu.VMEM)
    return pl.pallas_call(
        step_kernel,
        out_shape=(
            jax.ShapeDtypeStruct((fine_total, width), f32),
            jax.ShapeDtypeStruct((mid_dev, width), f32),
            jax.ShapeDtypeStruct((coarse_total, width), f32),
            jax.ShapeDtypeStruct((row_count, width), bf16),
        ),
        in_specs=[vmem, vmem, vmem, pl.BlockSpec(memory_space=pltpu.SMEM)] + [vmem] * 4,
        out_specs=(vmem,) * 4,
        scratch_shapes=[pltpu.VMEM(moved, bf16)] * 8
        + [
            pltpu.VMEM((chunks + 1, slots, lanes), f32),
            pltpu.VMEM((chunks, slots, lanes), f32),
            pltpu.VMEM((cells, fine, 2 * 128), bf16),
            pltpu.VMEM((fine_total, width + lanes), bf16),
            pltpu.VMEM((row_count, slots), bf16),
            pltpu.VMEM((4, 8, 1, lanes), jnp.int32),
            pltpu.VMEM((4, 4, mid_dev, width), bf16),
            pltpu.VMEM((4, 4, mid_dev, width), bf16),
        ]
        + [pltpu.VMEM((4, 4, mid_dev, split), bf16)] * 4
        + [pltpu.VMEM((4, mid_dev, split), bf16)] * 4
        + [pltpu.VMEM((4, 4, 1, lanes), f32)] * 4
        + [pltpu.VMEM((4, 1, lanes), f32)] * 2
        + [pltpu.VMEM((8,) + eighth, f32)] * 2
        + [pltpu.VMEM((4,) + eighth, f32)] * 2
        + [
            pltpu.VMEM((8,) + eighth, f32),
            pltpu.SemaphoreType.DMA((copies,)),
            pltpu.SemaphoreType.DMA((copies,)),
        ],
        compiler_params=pltpu.CompilerParams(
            collective_id=0, has_side_effects=True, vmem_limit_bytes=60 * 1024 * 1024
        ),
        name="lloyd_step",
    )(
        samples,
        cell_of_row.reshape(1, row_count),
        fine_centroids,
        sharpness,
        mid_of_fine.reshape(1, fine_total),
        mid_centroids,
        jnp.pad(coarse_of_mid, (0, lanes - mid_dev))[None],
        coarse_centroids,
    )


def solution(mesh):
    split = Mesh(
        mesh.devices.reshape(mesh.shape["group"], 4, 4, 2),
        ("group", "member_0", "member_1", "member_2"),
    )
    placed = (
        P(GROUP_MEMBER, None),
        P(GROUP_MEMBER, None),
        P(GROUP_MEMBER, None),
        P(GROUP_MEMBER),
        P(GROUP_MEMBER),
        P(GROUP_MEMBER, None),
        P(GROUP_MEMBER),
        P(),
    )
    return jax.shard_map(
        shards,
        mesh=split,
        in_specs=placed,
        out_specs=(P(GROUP_MEMBER, None), P(GROUP_MEMBER, None), P(), P(GROUP_MEMBER, None)),
        check_vma=False,
    )
```

```python
import math

import jax
import jax.numpy as jnp
from jax import lax
from jax.experimental import pallas as pl
from jax.experimental.pallas import tpu as pltpu
from jax.sharding import Mesh
from jax.sharding import PartitionSpec as P

MEMBER = ("member_0", "member_1", "member_2")
GROUP_MEMBER = ("group", "member_0", "member_1", "member_2")
RINGS = ("group", "member_0", "member_1")
CORE = "member_2"
EMPTY = 64.0
MESH_ID = pl.DeviceIdType.MESH


class Wires:
    def __init__(self, send_sem, recv_sem):
        self.send_sem, self.recv_sem = send_sem, recv_sem
        self.arrivals, self.leave = 0, []
        self.other = 1 - lax.axis_index(CORE)

    def leaving(self, like):
        self.leave.append(like)
        return len(self.leave) - 1

    def landing(self):
        self.arrivals += 1
        return self.arrivals - 1

    def copy(self, source, target, to, send_at, recv_at):
        return pltpu.make_async_remote_copy(
            src_ref=source,
            dst_ref=target,
            send_sem=self.send_sem.at[send_at],
            recv_sem=self.recv_sem.at[recv_at],
            device_id=to,
            device_id_type=MESH_ID,
        )

    def send(self, source, target, to, send_at, recv_at):
        self.copy(source, target, to, send_at, recv_at).start()

    def landed(self, like, recv_at):
        self.copy(like, like, {CORE: self.other}, 0, recv_at).wait_recv()

    def drain(self):
        for at, like in enumerate(self.leave):
            self.copy(like, like, {CORE: self.other}, at, 0).wait_send()


def greet(peers):
    for peer in peers:
        pl.semaphore_signal(
            pltpu.get_barrier_semaphore(), inc=1, device_id=peer, device_id_type=MESH_ID
        )


def greeted(peers):
    pl.semaphore_wait(pltpu.get_barrier_semaphore(), len(peers))


def ring_places(axis):
    me = lax.axis_index(axis)
    return me, lax.rem(me + 1, 4), lax.rem(me + 3, 4), lax.rem(me + 2, 4)


def ring_peers(both_cores):
    core = lax.axis_index(CORE)
    peers = [{CORE: 1 - core}]
    for axis in RINGS:
        for to in ring_places(axis)[1:]:
            peers.append({axis: to})
            if both_cores:
                peers.append({axis: to, CORE: 1 - core})
    return peers


class Exchange:
    def __init__(self, wires, refs):
        self.wires, self.refs = wires, refs
        self.core = lax.axis_index(CORE)
        self.rings = [ring_places(axis) for axis in RINGS]
        self.chunks = range(refs[0].shape[0])
        self.leave = [wires.leaving(ref.at[:, pl.ds(0, 3)]) for ref in refs[:3]]
        self.leave.append(wires.leaving(refs[2].at[:, 0, :, :, 0]))
        self.land = [[wires.landing() for _ in self.chunks] for _ in range(4)]

    def spot(self, chunk, dim, index, core_at=slice(None)):
        at = [chunk, slice(None), slice(None), slice(None), core_at]
        at[dim + 1] = index
        return tuple(at)

    def start(self, phase, chunk):
        wires, core, other = self.wires, self.core, 1 - self.core
        dim = (chunk + phase) % 3
        source, target = self.refs[phase], self.refs[phase + 1]
        axis = RINGS[dim]
        me, up, down, across = self.rings[dim]
        leave, land = self.leave[phase], self.land[phase][chunk]
        if phase < 2:
            for to in (across, up, down):
                wires.send(
                    source.at[self.spot(chunk, dim, to)],
                    target.at[self.spot(chunk, dim, me)],
                    {axis: to},
                    leave,
                    land,
                )
            own = self.spot(chunk, dim, me)
        else:
            own = self.spot(chunk, dim, me, core)
            for to in (across, up, down):
                for core_at in (0, 1):
                    wires.send(
                        source.at[self.spot(chunk, dim, to, core_at)],
                        target.at[own],
                        {axis: to, CORE: core_at},
                        leave,
                        land,
                    )
            wires.send(
                source.at[self.spot(chunk, dim, me, other)],
                target.at[own],
                {CORE: other},
                self.leave[3],
                self.land[3][chunk],
            )
        target[own] = source[own]

    def finish(self, phase, chunk):
        target = self.refs[phase + 1]
        self.wires.landed(target.at[chunk, pl.ds(0, 3)], self.land[phase][chunk])
        if phase == 2:
            self.wires.landed(target.at[chunk, 0, :, :, 0], self.land[3][chunk])

    def advance(self, phase, chunks=None):
        for chunk in self.chunks if chunks is None else chunks:
            self.finish(phase, chunk)
            if phase < 2:
                self.start(phase + 1, chunk)


class Octet:
    def __init__(self, wires):
        self.wires = wires
        self.me = lax.axis_index("member_0") * 2 + lax.axis_index(CORE)

    def start(self, source_of, targets):
        self.like = targets.at[pl.ds(0, 7)]
        leave, self.land = self.wires.leaving(self.like), self.wires.landing()
        for step in range(1, 8):
            to = lax.rem(self.me + step, 8)
            where = {"member_0": to // 2, CORE: lax.rem(to, 2)}
            self.wires.send(source_of(to), targets.at[self.me], where, leave, self.land)

    def finish(self):
        self.wires.landed(self.like, self.land)


class Ring:
    def __init__(self, wires, axis):
        self.wires, self.axis = wires, axis
        self.me, self.up, self.down, self.across = ring_places(axis)

    def order(self):
        return (self.across, self.up, self.down)

    def open(self, targets):
        self.like, self.target = targets.at[pl.ds(0, 3)], targets.at[self.me]
        self.leave, self.land = self.wires.leaving(self.like), self.wires.landing()

    def send(self, way, source):
        self.wires.send(
            source, self.target, {self.axis: self.order()[way]}, self.leave, self.land
        )

    def start(self, source_of, targets):
        self.open(targets)
        for way, to in enumerate(self.order()):
            self.send(way, source_of(to))

    def finish(self):
        self.wires.landed(self.like, self.land)


def diagonal(rows, lanes):
    return lax.broadcasted_iota(jnp.int32, (rows, lanes), 0) == lax.broadcasted_iota(
        jnp.int32, (rows, lanes), 1
    )


def as_column(row, rows):
    return jnp.sum(
        jnp.where(diagonal(rows, row.shape[1]), row, jnp.zeros_like(row)), axis=1, keepdims=True
    )


def step_kernel(
    samples_in,
    cell_in,
    fine_in,
    sharp_ref,
    mid_in,
    mids_in,
    route_in,
    coarse_in,
    fine_new_ref,
    mids_new_ref,
    coarse_new_ref,
    rec_ref,
    outgoing,
    there_a,
    there_b,
    arrived,
    rebuilt,
    back_a,
    back_b,
    returned,
    wide,
    back,
    resps,
    sums,
    chosen,
    maps,
    give,
    core_in,
    half_a,
    half_b,
    near_a,
    near_b,
    line_a,
    line_b,
    far_a,
    far_b,
    give_m,
    core_m,
    half_m,
    near_m,
    line_m,
    far_m,
    part_c,
    first_sum,
    second_sum,
    third_sum,
    total,
    samples_ref,
    cell_ref,
    fine_ref,
    mid_ref,
    mids_ref,
    route_ref,
    coarse_ref,
    route_wide,
    load_sem,
    send_sem,
    recv_sem,
):
    f32, bf16 = jnp.float32, jnp.bfloat16
    loads = [
        pltpu.make_async_copy(source, target, load_sem.at[at])
        for at, (source, target) in enumerate(
            (
                (cell_in, cell_ref),
                (samples_in, samples_ref),
                (route_in, route_ref),
                (fine_in, fine_ref),
                (mid_in, mid_ref),
                (mids_in, mids_ref),
                (coarse_in, coarse_ref),
            )
        )
    ]
    for load in loads:
        load.start()
    wires = Wires(send_sem, recv_sem)
    core = lax.axis_index(CORE)
    other = 1 - core
    chunks, lanes = outgoing.shape[0], outgoing.shape[-1]
    row_count, width = samples_ref.shape
    slots = chosen.shape[1]
    cells = sharp_ref.shape[0]
    fine = fine_ref.shape[0] // cells
    per_source = 2 * cells
    sources = slots // per_source
    mid_dev = mids_ref.shape[0]
    split = half_a.shape[-1]

    peers = ring_peers(True)
    greet(peers)
    loads[0].wait()
    cell_row = cell_ref[...]
    cell_column = as_column(cell_row, row_count)
    earlier = lax.broadcasted_iota(jnp.int32, (row_count, row_count), 0) < lax.broadcasted_iota(
        jnp.int32, (row_count, row_count), 1
    )
    rank = jnp.sum(
        jnp.where((cell_column == cell_row) & earlier, 1, 0), axis=0, keepdims=True
    )
    slot_row = cell_row * 2 + rank
    place = lax.broadcasted_iota(jnp.int32, (slots, row_count), 0)
    picked = jnp.where(place == slot_row, 1.0, 0.0).astype(bf16)
    used = jnp.dot(picked, jnp.ones((row_count, lanes), bf16), preferred_element_type=f32) > 0.5

    for load in loads[1:]:
        load.wait()
    route_wide[...] = jnp.zeros_like(route_wide)
    route_wide[:, pl.ds(0, mid_dev)] = route_ref[...]
    greeted(peers)
    moving = Exchange(wires, (outgoing, there_a, there_b, arrived))
    for chunk in range(0, chunks, 2):
        lines = jnp.dot(
            picked, samples_ref[:, pl.ds(chunk * lanes, 2 * lanes)], preferred_element_type=f32
        )
        for at in range(2):
            line = jnp.where(used, lines[:, at * lanes : (at + 1) * lanes], EMPTY)
            outgoing[chunk + at] = line.reshape(outgoing.shape[1:]).astype(bf16)
            moving.start(0, chunk + at)
    octet = Octet(wires)
    xs, zs, ys = Ring(wires, "member_0"), Ring(wires, "member_1"), Ring(wires, "group")
    maps_ring = Ring(wires, "member_1")
    octet.start(lambda to: route_wide, maps.at[zs.me])
    maps[zs.me, octet.me] = route_wide[...]
    slot_column = as_column(slot_row, row_count)
    along = lax.broadcasted_iota(jnp.int32, (row_count, slots), 1)
    chosen[...] = jnp.where(along == slot_column, 1.0, 0.0).astype(bf16)
    moving.advance(0)
    octet.finish()
    maps_ring.start(lambda to: maps.at[zs.me], maps)
    moving.advance(1)
    moving.advance(2)
    maps_ring.finish()

    for chunk in range(chunks):
        piece = arrived[chunk].astype(f32).reshape(slots, lanes)
        wide[chunk] = jnp.where(piece > 0.5 * EMPTY, 0.0, piece)
        if chunk == 0:
            wide[chunks] = jnp.where(piece > 0.5 * EMPTY, 0.0, 1.0)

    def cell_rows(cell, number):
        spots = [pl.ds(cell * 2 + most, sources, stride=per_source) for most in range(2)]
        return jnp.concatenate(
            [
                jnp.concatenate([wide[chunk, at, :] for at in spots], axis=0).astype(bf16)
                for chunk in range(number)
            ],
            axis=1,
        )

    for cell in range(cells):
        centres = fine_ref[pl.ds(cell * fine, fine), :]
        centres_wide = centres.astype(f32)
        norms = jnp.sum(centres_wide * centres_wide, axis=1, keepdims=True)
        products = lax.dot_general(
            centres,
            cell_rows(cell, chunks),
            (((1,), (1,)), ((), ())),
            preferred_element_type=f32,
        )
        scores = (products - 0.5 * norms) * (sharp_ref[cell] / math.sqrt(width))
        exponent = jnp.exp(scores - jnp.max(scores, axis=0, keepdims=True))
        resp = (exponent / jnp.sum(exponent, axis=0, keepdims=True)).astype(bf16)
        resps[cell] = resp
        lines = lax.dot_general(resp, centres, (((0,), (0,)), ((), ())), preferred_element_type=f32)
        for chunk in range(chunks):
            for most in range(2):
                back[chunk, pl.ds(cell * 2 + most, sources, stride=per_source), :] = lines[
                    most * sources : (most + 1) * sources, chunk * lanes : (chunk + 1) * lanes
                ]
    homing = Exchange(wires, (rebuilt, back_a, back_b, returned))
    for chunk in range(chunks):
        rebuilt[chunk] = back[chunk].reshape(rebuilt.shape[1:]).astype(bf16)
        homing.start(0, chunk)

    for cell in range(cells):
        here = pl.ds(cell * fine, fine)
        weighted = jnp.dot(resps[cell], cell_rows(cell, chunks + 1), preferred_element_type=f32)
        sums[here, :] = weighted.astype(bf16)
        centres_wide = fine_ref[here, :].astype(f32)
        share = 1.0 / (weighted[:, width:] + 1.0)
        for chunk in range(chunks):
            at = slice(chunk * lanes, (chunk + 1) * lanes)
            fine_new_ref[here, pl.ds(chunk * lanes, lanes)] = (
                weighted[:, at] + centres_wide[:, at]
            ) * share

    rows_of = 4 * mid_dev
    local_mid = mid_ref[...] - lax.axis_index("group") * (32 * mid_dev)
    spread = lax.broadcasted_iota(jnp.int32, (rows_of, fine_ref.shape[0]), 0)
    spread = (spread // mid_dev) * (2 * mid_dev) + spread % mid_dev

    def mid_part(x, core_at):
        wanted = local_mid - (x * 8 + core_at) * mid_dev
        picker = jnp.where(spread == wanted, 1.0, 0.0).astype(bf16)
        return jnp.dot(picker, sums[...], preferred_element_type=f32)

    def mass_row(part, z):
        tile = part[z * mid_dev : (z + 1) * mid_dev, width:]
        return jnp.sum(
            jnp.where(diagonal(mid_dev, lanes), tile, 0.0), axis=0, keepdims=True
        )

    order_x = xs.order() + (xs.me,)
    swap = [wires.landing() for _ in range(4)]
    swap_m = [wires.landing() for _ in range(4)]
    leave, leave_m = wires.leaving(give), wires.leaving(give_m)
    for way, x in enumerate(order_x):
        part = mid_part(x, other)
        for z in range(4):
            give[x, z] = part[z * mid_dev : (z + 1) * mid_dev, :width].astype(bf16)
            give_m[x, z] = mass_row(part, z)
        wires.send(give.at[x], core_in.at[x], {CORE: other}, leave, swap[way])
        wires.send(give_m.at[x], core_m.at[x], {CORE: other}, leave_m, swap_m[way])
    xs_m = Ring(wires, "member_0")
    xs.open(near_a)
    xs_m.open(near_m)
    level = lax.broadcasted_iota(jnp.int32, (coarse_ref.shape[0], lanes), 0)
    coarse_part = jnp.zeros((coarse_ref.shape[0], width), f32)
    coarse_mass = jnp.zeros((coarse_ref.shape[0], lanes), f32)
    for way, x in enumerate(order_x):
        part = mid_part(x, core)
        wires.landed(core_in.at[x], swap[way])
        wires.landed(core_m.at[x], swap_m[way])
        for z in range(4):
            half = part[z * mid_dev : (z + 1) * mid_dev, :width] + core_in[x, z].astype(f32)
            half = half.astype(bf16)
            half_a[x, z] = half[:, :split]
            half_b[z, x] = half[:, split:]
            masses = mass_row(part, z) + core_m[x, z]
            half_m[x, z] = masses
            goes = level == maps[z, x * 2 + core]
            coarse_mass += jnp.where(goes, masses, 0.0)
            coarse_part += jnp.dot(
                jnp.where(goes, 1.0, 0.0).astype(bf16)[:, :mid_dev],
                half,
                preferred_element_type=f32,
            )
        if way < 3:
            xs.send(way, half_a.at[x])
            xs_m.send(way, half_m.at[x])
    zs.start(lambda to: half_b.at[to], near_b)
    coarse_mass = jnp.broadcast_to(jnp.sum(coarse_mass, axis=1, keepdims=True), coarse_mass.shape)
    for at in range(8):
        part_c[at, :, pl.ds(0, width)] = coarse_part[8 * at : 8 * at + 8].astype(bf16)
        part_c[at, :, pl.ds(width, lanes)] = coarse_mass[8 * at : 8 * at + 8].astype(bf16)
    octet.start(lambda to: part_c.at[to], first_sum)
    first_sum[octet.me] = part_c[octet.me]

    homing.advance(0)
    homing.advance(1, (2, 5))

    xs.finish()
    xs_m.finish()
    octet.finish()
    second_sum[zs.me] = sum(first_sum[at].astype(f32) for at in range(8))
    zs_coarse = Ring(wires, "member_1")
    zs_coarse.start(lambda to: second_sum.at[zs.me], second_sum)
    for z in range(4):
        line_a[z] = (
            half_a[xs.me, z].astype(f32) + sum(near_a[at, z].astype(f32) for at in xs.order())
        ).astype(bf16)
        line_m[z] = half_m[xs.me, z] + sum(near_m[at, z] for at in xs.order())
    zs_late, zs_m, xs_late = Ring(wires, "member_1"), Ring(wires, "member_1"), Ring(wires, "member_0")
    zs_late.start(lambda to: line_a.at[to], far_a)
    zs_m.start(lambda to: line_m.at[to], far_m)
    zs.finish()
    for x in range(4):
        line_b[x] = (
            half_b[zs.me, x].astype(f32) + sum(near_b[at, x].astype(f32) for at in zs.order())
        ).astype(bf16)
    xs_late.start(lambda to: line_b.at[to], far_b)

    homing.advance(1, (0, 3))
    zs_coarse.finish()
    third_sum[ys.me] = sum(second_sum[at] for at in range(4))
    ys.start(lambda to: third_sum.at[ys.me], third_sum)
    homing.advance(1, (1, 4))

    ys.finish()
    total[octet.me] = sum(third_sum[at] for at in range(4)).astype(bf16)
    octet.start(lambda to: total.at[octet.me], total)

    def reconstruct(pair):
        homing.advance(2, pair)
        lines = jnp.concatenate(
            [returned[chunk].astype(f32).reshape(slots, lanes).astype(bf16) for chunk in pair],
            axis=1,
        )
        lines = jnp.dot(chosen[...], lines, preferred_element_type=f32).astype(bf16)
        for at, chunk in enumerate(pair):
            rec_ref[:, pl.ds(chunk * lanes, lanes)] = lines[:, at * lanes : (at + 1) * lanes]

    reconstruct((2, 5))
    zs_late.finish()
    zs_m.finish()
    xs_late.finish()
    masses = line_m[zs.me] + sum(far_m[at] for at in zs.order())
    share = 1.0 / (as_column(masses, mid_dev) + 1.0)
    own_a = line_a[zs.me].astype(f32) + sum(far_a[at].astype(f32) for at in zs.order())
    own_b = line_b[xs.me].astype(f32) + sum(far_b[at].astype(f32) for at in xs.order())
    mids_new_ref[:, pl.ds(0, split)] = (own_a + mids_ref[:, pl.ds(0, split)]) * share
    mids_new_ref[:, pl.ds(split, split)] = (own_b + mids_ref[:, pl.ds(split, split)]) * share

    reconstruct((0, 3))
    reconstruct((1, 4))

    octet.finish()
    for at in range(8):
        here = pl.ds(8 * at, 8)
        share = 1.0 / (total[at, :, pl.ds(width, lanes)].astype(f32) + 1.0)
        for chunk in range(chunks):
            there = pl.ds(chunk * lanes, lanes)
            coarse_new_ref[here, there] = (
                total[at, :, there].astype(f32) + coarse_ref[here, there]
            ) * share
    wires.drain()


def shards(
    samples,
    cell_of_row,
    fine_centroids,
    sharpness,
    mid_of_fine,
    mid_centroids,
    coarse_of_mid,
    coarse_centroids,
):
    row_count, width = samples.shape
    cells = sharpness.shape[0]
    fine_total = fine_centroids.shape[0]
    fine = fine_total // cells
    mid_dev = mid_centroids.shape[0]
    coarse_total = coarse_centroids.shape[0]
    lanes = 128
    chunks = width // lanes
    slots = 128 * 2 * cells
    split = width // 2
    moved = (chunks, 4, 4, 4, 2, 2 * cells, lanes)
    eighth = (coarse_total // 8, width + lanes)
    leaves, lands = 2 * 4 + 3 + 9 + 2, 2 * 4 * chunks + 3 + 9 + 8
    f32, bf16 = jnp.float32, jnp.bfloat16
    vmem = pl.BlockSpec(memory_space=pltpu.VMEM)
    hbm = pl.BlockSpec(memory_space=pltpu.HBM)
    results = pl.pallas_call(
        step_kernel,
        out_shape=(
            pltpu.VMEM((fine_total, width), f32),
            pltpu.VMEM((mid_dev, width), f32),
            pltpu.VMEM((coarse_total, width), f32),
            pltpu.VMEM((row_count, width), bf16),
        ),
        in_specs=[hbm] * 3 + [pl.BlockSpec(memory_space=pltpu.SMEM)] + [hbm] * 4,
        out_specs=(vmem,) * 4,
        scratch_shapes=[pltpu.VMEM(moved, bf16)] * 8
        + [
            pltpu.VMEM((chunks + 1, slots, lanes), f32),
            pltpu.VMEM((chunks, slots, lanes), f32),
            pltpu.VMEM((cells, fine, 2 * 128), bf16),
            pltpu.VMEM((fine_total, width + lanes), bf16),
            pltpu.VMEM((row_count, slots), bf16),
            pltpu.VMEM((4, 8, 1, lanes), jnp.int32),
            pltpu.VMEM((4, 4, mid_dev, width), bf16),
            pltpu.VMEM((4, 4, mid_dev, width), bf16),
        ]
        + [pltpu.VMEM((4, 4, mid_dev, split), bf16)] * 4
        + [pltpu.VMEM((4, mid_dev, split), bf16)] * 4
        + [pltpu.VMEM((4, 4, 1, lanes), f32)] * 4
        + [pltpu.VMEM((4, 1, lanes), f32)] * 2
        + [pltpu.VMEM((8,) + eighth, bf16)] * 2
        + [pltpu.VMEM((4,) + eighth, f32)] * 2
        + [
            pltpu.VMEM((8,) + eighth, bf16),
            pltpu.VMEM((row_count, width), bf16),
            pltpu.VMEM((1, row_count), jnp.int32),
            pltpu.VMEM((fine_total, width), bf16),
            pltpu.VMEM((1, fine_total), jnp.int32),
            pltpu.VMEM((mid_dev, width), f32),
            pltpu.VMEM((1, mid_dev), jnp.int32),
            pltpu.VMEM((coarse_total, width), f32),
            pltpu.VMEM((1, lanes), jnp.int32),
            pltpu.SemaphoreType.DMA((7,)),
            pltpu.SemaphoreType.DMA((leaves,)),
            pltpu.SemaphoreType.DMA((lands,)),
        ],
        compiler_params=pltpu.CompilerParams(
            collective_id=0, has_side_effects=True, vmem_limit_bytes=54 * 1024 * 1024
        ),
        name="lloyd_step",
    )(
        samples,
        cell_of_row.reshape(1, row_count),
        fine_centroids,
        sharpness,
        mid_of_fine.reshape(1, fine_total),
        mid_centroids,
        coarse_of_mid.reshape(1, mid_dev),
        coarse_centroids,
    )
    return pl.pallas_call(
        put_out_kernel,
        out_shape=tuple(jax.ShapeDtypeStruct(one.shape, one.dtype) for one in results),
        in_specs=[vmem] * 4,
        out_specs=(hbm,) * 4,
        scratch_shapes=[pltpu.SemaphoreType.DMA((4,))],
        compiler_params=pltpu.CompilerParams(vmem_limit_bytes=1024 * 1024),
        name="put_out",
    )(*results)


def put_out_kernel(*refs):
    copies = [
        pltpu.make_async_copy(source, target, refs[8].at[at])
        for at, (source, target) in enumerate(zip(refs[:4], refs[4:8]))
    ]
    for copy in copies:
        copy.start()
    for copy in copies:
        copy.wait()


def solution(mesh):
    split = Mesh(
        mesh.devices.reshape(mesh.shape["group"], 4, 4, 2),
        ("group", "member_0", "member_1", "member_2"),
    )
    placed = (
        P(GROUP_MEMBER, None),
        P(GROUP_MEMBER, None),
        P(GROUP_MEMBER, None),
        P(GROUP_MEMBER),
        P(GROUP_MEMBER),
        P(GROUP_MEMBER, None),
        P(GROUP_MEMBER),
        P(),
    )
    return jax.shard_map(
        shards,
        mesh=split,
        in_specs=placed,
        out_specs=(P(GROUP_MEMBER, None), P(GROUP_MEMBER, None), P(), P(GROUP_MEMBER, None)),
        check_vma=False,
    )
```

```python
import math

import jax
import jax.numpy as jnp
from jax import lax
from jax.experimental import pallas as pl
from jax.experimental.pallas import tpu as pltpu
from jax.sharding import Mesh
from jax.sharding import PartitionSpec as P

MEMBER = ("member_0", "member_1", "member_2")
GROUP_MEMBER = ("group", "member_0", "member_1", "member_2")
RINGS = ("group", "member_0", "member_1")
CORE = "member_2"
EMPTY = 64.0
MESH_ID = pl.DeviceIdType.MESH


class Wires:
    def __init__(self, send_sem, recv_sem):
        self.send_sem, self.recv_sem = send_sem, recv_sem
        self.arrivals, self.leave = 0, []
        self.other = 1 - lax.axis_index(CORE)

    def leaving(self, like):
        self.leave.append(like)
        return len(self.leave) - 1

    def landing(self):
        self.arrivals += 1
        return self.arrivals - 1

    def copy(self, source, target, to, send_at, recv_at):
        return pltpu.make_async_remote_copy(
            src_ref=source,
            dst_ref=target,
            send_sem=self.send_sem.at[send_at],
            recv_sem=self.recv_sem.at[recv_at],
            device_id=to,
            device_id_type=MESH_ID,
        )

    def send(self, source, target, to, send_at, recv_at):
        self.copy(source, target, to, send_at, recv_at).start()

    def landed(self, like, recv_at):
        self.copy(like, like, {CORE: self.other}, 0, recv_at).wait_recv()

    def drain(self):
        for at, like in enumerate(self.leave):
            self.copy(like, like, {CORE: self.other}, at, 0).wait_send()


def greet(peers):
    for peer in peers:
        pl.semaphore_signal(
            pltpu.get_barrier_semaphore(), inc=1, device_id=peer, device_id_type=MESH_ID
        )


def greeted(peers):
    pl.semaphore_wait(pltpu.get_barrier_semaphore(), len(peers))


def ring_places(axis):
    me = lax.axis_index(axis)
    return me, lax.rem(me + 1, 4), lax.rem(me + 3, 4), lax.rem(me + 2, 4)


def ring_peers(both_cores):
    core = lax.axis_index(CORE)
    peers = [{CORE: 1 - core}]
    for axis in RINGS:
        for to in ring_places(axis)[1:]:
            peers.append({axis: to})
            if both_cores:
                peers.append({axis: to, CORE: 1 - core})
    return peers


class Exchange:
    def __init__(self, wires, refs):
        self.wires, self.refs = wires, refs
        self.core = lax.axis_index(CORE)
        self.rings = [ring_places(axis) for axis in RINGS]
        self.chunks = range(refs[0].shape[0])
        self.leave = [wires.leaving(ref.at[:, pl.ds(0, 3)]) for ref in refs[:3]]
        self.leave.append(wires.leaving(refs[2].at[:, 0, :, :, 0]))
        self.land = [[wires.landing() for _ in self.chunks] for _ in range(4)]

    def spot(self, chunk, dim, index, core_at=slice(None)):
        at = [chunk, slice(None), slice(None), slice(None), core_at]
        at[dim + 1] = index
        return tuple(at)

    def start(self, phase, chunk):
        wires, core, other = self.wires, self.core, 1 - self.core
        dim = (chunk + phase) % 3
        source, target = self.refs[phase], self.refs[phase + 1]
        axis = RINGS[dim]
        me, up, down, across = self.rings[dim]
        leave, land = self.leave[phase], self.land[phase][chunk]
        if phase < 2:
            for to in (across, up, down):
                wires.send(
                    source.at[self.spot(chunk, dim, to)],
                    target.at[self.spot(chunk, dim, me)],
                    {axis: to},
                    leave,
                    land,
                )
            own = self.spot(chunk, dim, me)
        else:
            own = self.spot(chunk, dim, me, core)
            for to in (across, up, down):
                for core_at in (0, 1):
                    wires.send(
                        source.at[self.spot(chunk, dim, to, core_at)],
                        target.at[own],
                        {axis: to, CORE: core_at},
                        leave,
                        land,
                    )
            wires.send(
                source.at[self.spot(chunk, dim, me, other)],
                target.at[own],
                {CORE: other},
                self.leave[3],
                self.land[3][chunk],
            )
        target[own] = source[own]

    def finish(self, phase, chunk):
        target = self.refs[phase + 1]
        self.wires.landed(target.at[chunk, pl.ds(0, 3)], self.land[phase][chunk])
        if phase == 2:
            self.wires.landed(target.at[chunk, 0, :, :, 0], self.land[3][chunk])

    def advance(self, phase, chunks=None):
        for chunk in self.chunks if chunks is None else chunks:
            self.finish(phase, chunk)
            if phase < 2:
                self.start(phase + 1, chunk)


class Octet:
    def __init__(self, wires):
        self.wires = wires
        self.me = lax.axis_index("member_0") * 2 + lax.axis_index(CORE)

    def start(self, source_of, targets):
        self.like = targets.at[pl.ds(0, 7)]
        leave, self.land = self.wires.leaving(self.like), self.wires.landing()
        for step in range(1, 8):
            to = lax.rem(self.me + step, 8)
            where = {"member_0": to // 2, CORE: lax.rem(to, 2)}
            self.wires.send(source_of(to), targets.at[self.me], where, leave, self.land)

    def finish(self):
        self.wires.landed(self.like, self.land)


class Ring:
    def __init__(self, wires, axis):
        self.wires, self.axis = wires, axis
        self.me, self.up, self.down, self.across = ring_places(axis)

    def order(self):
        return (self.across, self.up, self.down)

    def open(self, targets):
        self.like, self.target = targets.at[pl.ds(0, 3)], targets.at[self.me]
        self.leave, self.land = self.wires.leaving(self.like), self.wires.landing()

    def send(self, way, source):
        self.wires.send(
            source, self.target, {self.axis: self.order()[way]}, self.leave, self.land
        )

    def start(self, source_of, targets):
        self.open(targets)
        for way, to in enumerate(self.order()):
            self.send(way, source_of(to))

    def finish(self):
        self.wires.landed(self.like, self.land)


class Halves:
    def __init__(self, wires, ring, relay, near):
        self.wires, self.ring, self.relay, self.near = wires, ring, relay, near
        self.leave_relay, self.leave_near = wires.leaving(relay), wires.leaving(near)
        self.land_relay = [wires.landing() for _ in range(2)]
        self.land_near = wires.landing()

    def send_near(self, blocks, way, half):
        to = (self.ring.up, self.ring.down)[way]
        part = pl.ds(2 * half, 2)
        self.wires.send(
            blocks.at[to, part],
            self.near.at[way, part],
            {self.ring.axis: to},
            self.leave_near,
            self.land_near,
        )

    def offer(self, step, blocks):
        if step > 0:
            self.send_near(blocks, step - 1, 2 - step)
            return
        for way, to in enumerate((self.ring.up, self.ring.down)):
            self.wires.send(
                blocks.at[self.ring.across, pl.ds(2 * way, 2)],
                self.relay.at[way],
                {self.ring.axis: to},
                self.leave_relay,
                self.land_relay[way],
            )

    def pass_on(self, blocks):
        for way, to in enumerate((self.ring.up, self.ring.down)):
            self.wires.landed(self.relay.at[way], self.land_relay[way])
            for at in range(2):
                blocks[to, 2 * way + at] = (
                    blocks[to, 2 * way + at].astype(jnp.float32)
                    + self.relay[way, at].astype(jnp.float32)
                ).astype(jnp.bfloat16)
            self.send_near(blocks, way, way)

    def finish(self):
        self.wires.landed(self.near, self.land_near)


def diagonal(rows, lanes):
    return lax.broadcasted_iota(jnp.int32, (rows, lanes), 0) == lax.broadcasted_iota(
        jnp.int32, (rows, lanes), 1
    )


def as_column(row, rows):
    return jnp.sum(
        jnp.where(diagonal(rows, row.shape[1]), row, jnp.zeros_like(row)), axis=1, keepdims=True
    )


def step_kernel(
    samples_in,
    cell_in,
    fine_in,
    sharp_ref,
    mid_in,
    mids_in,
    route_in,
    coarse_in,
    fine_new_ref,
    mids_new_ref,
    coarse_new_ref,
    rec_ref,
    outgoing,
    there_a,
    there_b,
    arrived,
    rebuilt,
    back_a,
    back_b,
    returned,
    wide,
    back,
    lines,
    products,
    norms,
    shares,
    turned,
    resps,
    sums,
    chosen,
    maps,
    give,
    core_in,
    half_a,
    half_b,
    near_a,
    near_b,
    relay_a,
    relay_b,
    line_a,
    line_b,
    far_a,
    far_b,
    give_m,
    core_m,
    half_m,
    near_m,
    line_m,
    far_m,
    part_c,
    first_sum,
    second_sum,
    third_sum,
    total,
    samples_ref,
    cell_ref,
    fine_ref,
    mid_ref,
    mids_ref,
    route_ref,
    coarse_ref,
    route_wide,
    load_sem,
    send_sem,
    recv_sem,
):
    f32, bf16 = jnp.float32, jnp.bfloat16
    loads = [
        pltpu.make_async_copy(source, target, load_sem.at[at])
        for at, (source, target) in enumerate(
            (
                (cell_in, cell_ref),
                (samples_in, samples_ref),
                (route_in, route_ref),
                (fine_in, fine_ref),
                (mid_in, mid_ref),
                (mids_in, mids_ref),
                (coarse_in, coarse_ref),
            )
        )
    ]
    for load in loads:
        load.start()
    wires = Wires(send_sem, recv_sem)
    core = lax.axis_index(CORE)
    other = 1 - core
    chunks, lanes = outgoing.shape[0], outgoing.shape[-1]
    row_count, width = samples_ref.shape
    slots = chosen.shape[1]
    cells = sharp_ref.shape[0]
    fine = fine_ref.shape[0] // cells
    per_source = 2 * cells
    sources = slots // per_source
    mid_dev = mids_ref.shape[0]
    split = half_a.shape[-1]

    peers = ring_peers(True)
    greet(peers)
    loads[0].wait()
    cell_row = cell_ref[...]
    cell_column = as_column(cell_row, row_count)
    earlier = lax.broadcasted_iota(jnp.int32, (row_count, row_count), 0) < lax.broadcasted_iota(
        jnp.int32, (row_count, row_count), 1
    )
    rank = jnp.sum(
        jnp.where((cell_column == cell_row) & earlier, 1, 0), axis=0, keepdims=True
    )
    slot_row = cell_row * 2 + rank
    place = lax.broadcasted_iota(jnp.int32, (slots, row_count), 0)
    picked = jnp.where(place == slot_row, 1.0, 0.0).astype(bf16)
    used = jnp.dot(picked, jnp.ones((row_count, lanes), bf16), preferred_element_type=f32) > 0.5

    for load in loads[1:]:
        load.wait()
    route_wide[...] = jnp.zeros_like(route_wide)
    route_wide[:, pl.ds(0, mid_dev)] = route_ref[...]
    greeted(peers)
    moving = Exchange(wires, (outgoing, there_a, there_b, arrived))
    for chunk in range(0, chunks, 2):
        put = jnp.dot(
            picked, samples_ref[:, pl.ds(chunk * lanes, 2 * lanes)], preferred_element_type=f32
        )
        for at in range(2):
            line = jnp.where(used, put[:, at * lanes : (at + 1) * lanes], EMPTY)
            outgoing[chunk + at] = line.reshape(outgoing.shape[1:]).astype(bf16)
            moving.start(0, chunk + at)
    octet = Octet(wires)
    xs, zs, ys = Ring(wires, "member_0"), Ring(wires, "member_1"), Ring(wires, "group")
    maps_ring = Ring(wires, "member_1")
    octet.start(lambda to: route_wide, maps.at[zs.me])
    maps[zs.me, octet.me] = route_wide[...]
    slot_column = as_column(slot_row, row_count)
    along = lax.broadcasted_iota(jnp.int32, (row_count, slots), 1)
    chosen[...] = jnp.where(along == slot_column, 1.0, 0.0).astype(bf16)
    moving.advance(0)
    octet.finish()
    maps_ring.start(lambda to: maps.at[zs.me], maps)
    for cell in range(cells):
        here = pl.ds(cell * fine, fine)
        centres_wide = fine_ref[here, :].astype(f32)
        norms[here, :] = jnp.broadcast_to(
            jnp.sum(centres_wide * centres_wide, axis=1, keepdims=True), (fine, lanes)
        )
    moving.advance(1)
    maps_ring.finish()

    for pair in range(0, chunks, 2):
        moving.advance(2, (pair, pair + 1))
        for chunk in (pair, pair + 1):
            piece = arrived[chunk].astype(f32).reshape(slots, lanes)
            wide[chunk] = jnp.where(piece > 0.5 * EMPTY, 0.0, piece)
            if chunk == 0:
                wide[chunks] = jnp.where(piece > 0.5 * EMPTY, 0.0, 1.0)
        at = pl.ds(pair * lanes, 2 * lanes)
        for cell in range(cells):
            spots = [pl.ds(cell * 2 + most, sources, stride=per_source) for most in range(2)]
            for chunk in (pair, pair + 1) + ((chunks,) if pair == 0 else ()):
                lines[cell, :, pl.ds(chunk * lanes, lanes)] = jnp.concatenate(
                    [wide[chunk, spot, :] for spot in spots], axis=0
                ).astype(bf16)
            product = lax.dot_general(
                fine_ref[pl.ds(cell * fine, fine), at],
                lines[cell, :, at],
                (((1,), (1,)), ((), ())),
                preferred_element_type=f32,
            )
            products[cell] = product if pair == 0 else products[cell] + product

    for cell in range(cells):
        half_norms = 0.5 * norms[pl.ds(cell * fine, fine), :]
        half_norms = jnp.concatenate([half_norms, half_norms], axis=1)
        scores = (products[cell] - half_norms) * (sharp_ref[cell] / math.sqrt(width))
        exponent = jnp.exp(scores - jnp.max(scores, axis=0, keepdims=True))
        resp = exponent / jnp.sum(exponent, axis=0, keepdims=True)
        resps[cell] = resp.astype(bf16)
        turned[cell] = resp.T.astype(bf16)
    homing = Exchange(wires, (rebuilt, back_a, back_b, returned))
    for pair in range(0, chunks, 2):
        for cell in range(cells):
            row = jnp.dot(
                turned[cell],
                fine_ref[pl.ds(cell * fine, fine), pl.ds(pair * lanes, 2 * lanes)],
                preferred_element_type=f32,
            )
            for at in range(2):
                for most in range(2):
                    back[pair + at, pl.ds(cell * 2 + most, sources, stride=per_source), :] = row[
                        most * sources : (most + 1) * sources, at * lanes : (at + 1) * lanes
                    ]
        for chunk in (pair, pair + 1):
            rebuilt[chunk] = back[chunk].reshape(rebuilt.shape[1:]).astype(bf16)
            homing.start(0, chunk)

    for cell in range(cells):
        here = pl.ds(cell * fine, fine)
        weighted = jnp.dot(resps[cell], lines[cell], preferred_element_type=f32)
        sums[here, :] = weighted.astype(bf16)
        fine_new_ref[here, :] = weighted[:, :width]
        shares[here, :] = 1.0 / (weighted[:, width:] + 1.0)

    rows_of = 4 * mid_dev
    local_mid = mid_ref[...] - lax.axis_index("group") * (32 * mid_dev)
    spread = lax.broadcasted_iota(jnp.int32, (rows_of, fine_ref.shape[0]), 0)
    spread = (spread // mid_dev) * (2 * mid_dev) + spread % mid_dev

    def mid_part(x, core_at):
        wanted = local_mid - (x * 8 + core_at) * mid_dev
        picker = jnp.where(spread == wanted, 1.0, 0.0).astype(bf16)
        return jnp.dot(picker, sums[...], preferred_element_type=f32)

    def mass_row(part, z):
        tile = part[z * mid_dev : (z + 1) * mid_dev, width:]
        return jnp.sum(
            jnp.where(diagonal(mid_dev, lanes), tile, 0.0), axis=0, keepdims=True
        )

    order_x = xs.order() + (xs.me,)
    swap = [wires.landing() for _ in range(4)]
    swap_m = [wires.landing() for _ in range(4)]
    leave, leave_m = wires.leaving(give), wires.leaving(give_m)
    for way, x in enumerate(order_x):
        part = mid_part(x, other)
        for z in range(4):
            give[x, z] = part[z * mid_dev : (z + 1) * mid_dev, :width].astype(bf16)
            give_m[x, z] = mass_row(part, z)
        wires.send(give.at[x], core_in.at[x], {CORE: other}, leave, swap[way])
        wires.send(give_m.at[x], core_m.at[x], {CORE: other}, leave_m, swap_m[way])
    xs_m = Ring(wires, "member_0")
    xs_m.open(near_m)
    ring_a, ring_b = Halves(wires, xs, relay_a, near_a), Halves(wires, zs, relay_b, near_b)
    level = lax.broadcasted_iota(jnp.int32, (coarse_ref.shape[0], lanes), 0)
    coarse_part = jnp.zeros((coarse_ref.shape[0], width), f32)
    coarse_mass = jnp.zeros((coarse_ref.shape[0], lanes), f32)
    for way, x in enumerate(order_x):
        part = mid_part(x, core)
        wires.landed(core_in.at[x], swap[way])
        wires.landed(core_m.at[x], swap_m[way])
        for z in range(4):
            half = part[z * mid_dev : (z + 1) * mid_dev, :width] + core_in[x, z].astype(f32)
            half = half.astype(bf16)
            half_a[x, z] = half[:, :split]
            half_b[z, x] = half[:, split:]
            masses = mass_row(part, z) + core_m[x, z]
            half_m[x, z] = masses
            goes = level == maps[z, x * 2 + core]
            coarse_mass += jnp.where(goes, masses, 0.0)
            coarse_part += jnp.dot(
                jnp.where(goes, 1.0, 0.0).astype(bf16)[:, :mid_dev],
                half,
                preferred_element_type=f32,
            )
        if way < 3:
            ring_a.offer(way, half_a)
            xs_m.send(way, half_m.at[x])
    ring_a.pass_on(half_a)
    for way in range(3):
        ring_b.offer(way, half_b)
    coarse_mass = jnp.broadcast_to(jnp.sum(coarse_mass, axis=1, keepdims=True), coarse_mass.shape)
    for at in range(8):
        part_c[at, :, pl.ds(0, width)] = coarse_part[8 * at : 8 * at + 8].astype(bf16)
        part_c[at, :, pl.ds(width, lanes)] = coarse_mass[8 * at : 8 * at + 8].astype(bf16)
    octet.start(lambda to: part_c.at[to], first_sum)
    first_sum[octet.me] = part_c[octet.me]

    homing.advance(0, (2, 5, 0, 3))
    ring_b.pass_on(half_b)
    homing.advance(0, (1, 4))
    for cell in range(cells):
        here = pl.ds(cell * fine, fine)
        for chunk in range(chunks):
            at = pl.ds(chunk * lanes, lanes)
            fine_new_ref[here, at] = (
                fine_new_ref[here, at] + fine_ref[here, at].astype(f32)
            ) * shares[here, :]
    ring_a.finish()
    xs_m.finish()
    octet.finish()
    second_sum[ys.me] = sum(first_sum[at].astype(f32) for at in range(8))
    ys.start(lambda to: second_sum.at[ys.me], second_sum)
    for z in range(4):
        line_a[z] = (
            half_a[xs.me, z].astype(f32) + near_a[0, z].astype(f32) + near_a[1, z].astype(f32)
        ).astype(bf16)
        line_m[z] = half_m[xs.me, z] + sum(near_m[at, z] for at in xs.order())
    zs_late, zs_m, xs_late = Ring(wires, "member_1"), Ring(wires, "member_1"), Ring(wires, "member_0")
    zs_late.start(lambda to: line_a.at[to], far_a)
    zs_m.start(lambda to: line_m.at[to], far_m)

    homing.advance(1, (2, 5))
    ys.finish()
    third_sum[zs.me] = sum(second_sum[at] for at in range(4))
    zs_coarse = Ring(wires, "member_1")
    zs_coarse.start(lambda to: third_sum.at[zs.me], third_sum)
    ring_b.finish()
    for x in range(4):
        line_b[x] = (
            half_b[zs.me, x].astype(f32) + near_b[0, x].astype(f32) + near_b[1, x].astype(f32)
        ).astype(bf16)
    xs_late.start(lambda to: line_b.at[to], far_b)

    homing.advance(1, (0, 3))
    homing.advance(1, (1, 4))
    zs_coarse.finish()
    total[octet.me] = sum(third_sum[at] for at in range(4)).astype(bf16)
    octet.start(lambda to: total.at[octet.me], total)

    def reconstruct(pair):
        homing.advance(2, pair)
        found = jnp.concatenate(
            [returned[chunk].astype(f32).reshape(slots, lanes).astype(bf16) for chunk in pair],
            axis=1,
        )
        found = jnp.dot(chosen[...], found, preferred_element_type=f32).astype(bf16)
        for at, chunk in enumerate(pair):
            rec_ref[:, pl.ds(chunk * lanes, lanes)] = found[:, at * lanes : (at + 1) * lanes]

    reconstruct((2, 5))
    zs_late.finish()
    zs_m.finish()
    xs_late.finish()
    masses = line_m[zs.me] + sum(far_m[at] for at in zs.order())
    share = 1.0 / (as_column(masses, mid_dev) + 1.0)
    own_a = line_a[zs.me].astype(f32) + sum(far_a[at].astype(f32) for at in zs.order())
    own_b = line_b[xs.me].astype(f32) + sum(far_b[at].astype(f32) for at in xs.order())
    mids_new_ref[:, pl.ds(0, split)] = (own_a + mids_ref[:, pl.ds(0, split)]) * share
    mids_new_ref[:, pl.ds(split, split)] = (own_b + mids_ref[:, pl.ds(split, split)]) * share

    reconstruct((0, 3))
    reconstruct((1, 4))

    octet.finish()
    for at in range(8):
        here = pl.ds(8 * at, 8)
        share = 1.0 / (total[at, :, pl.ds(width, lanes)].astype(f32) + 1.0)
        for chunk in range(chunks):
            there = pl.ds(chunk * lanes, lanes)
            coarse_new_ref[here, there] = (
                total[at, :, there].astype(f32) + coarse_ref[here, there]
            ) * share
    wires.drain()


def shards(
    samples,
    cell_of_row,
    fine_centroids,
    sharpness,
    mid_of_fine,
    mid_centroids,
    coarse_of_mid,
    coarse_centroids,
):
    row_count, width = samples.shape
    cells = sharpness.shape[0]
    fine_total = fine_centroids.shape[0]
    fine = fine_total // cells
    mid_dev = mid_centroids.shape[0]
    coarse_total = coarse_centroids.shape[0]
    lanes = 128
    chunks = width // lanes
    slots = 128 * 2 * cells
    split = width // 2
    moved = (chunks, 4, 4, 4, 2, 2 * cells, lanes)
    eighth = (coarse_total // 8, width + lanes)
    leaves, lands = 2 * 4 + 3 + 7 + 2 + 4, 2 * 4 * chunks + 3 + 7 + 8 + 6
    f32, bf16 = jnp.float32, jnp.bfloat16
    vmem = pl.BlockSpec(memory_space=pltpu.VMEM)
    hbm = pl.BlockSpec(memory_space=pltpu.HBM)
    results = pl.pallas_call(
        step_kernel,
        out_shape=(
            pltpu.VMEM((fine_total, width), f32),
            pltpu.VMEM((mid_dev, width), f32),
            pltpu.VMEM((coarse_total, width), f32),
            pltpu.VMEM((row_count, width), bf16),
        ),
        in_specs=[hbm] * 3 + [pl.BlockSpec(memory_space=pltpu.SMEM)] + [hbm] * 4,
        out_specs=(vmem,) * 4,
        scratch_shapes=[pltpu.VMEM(moved, bf16)] * 8
        + [
            pltpu.VMEM((chunks + 1, slots, lanes), f32),
            pltpu.VMEM((chunks, slots, lanes), f32),
            pltpu.VMEM((cells, 2 * 128, width + lanes), bf16),
            pltpu.VMEM((cells, fine, 2 * 128), f32),
            pltpu.VMEM((fine_total, lanes), f32),
            pltpu.VMEM((fine_total, lanes), f32),
            pltpu.VMEM((cells, 2 * 128, fine), bf16),
            pltpu.VMEM((cells, fine, 2 * 128), bf16),
            pltpu.VMEM((fine_total, width + lanes), bf16),
            pltpu.VMEM((row_count, slots), bf16),
            pltpu.VMEM((4, 8, 1, lanes), jnp.int32),
            pltpu.VMEM((4, 4, mid_dev, width), bf16),
            pltpu.VMEM((4, 4, mid_dev, width), bf16),
        ]
        + [pltpu.VMEM((4, 4, mid_dev, split), bf16)] * 2
        + [pltpu.VMEM((2, 4, mid_dev, split), bf16)] * 2
        + [pltpu.VMEM((2, 2, mid_dev, split), bf16)] * 2
        + [pltpu.VMEM((4, mid_dev, split), bf16)] * 4
        + [pltpu.VMEM((4, 4, 1, lanes), f32)] * 4
        + [pltpu.VMEM((4, 1, lanes), f32)] * 2
        + [pltpu.VMEM((8,) + eighth, bf16)] * 2
        + [pltpu.VMEM((4,) + eighth, f32)] * 2
        + [
            pltpu.VMEM((8,) + eighth, bf16),
            pltpu.VMEM((row_count, width), bf16),
            pltpu.VMEM((1, row_count), jnp.int32),
            pltpu.VMEM((fine_total, width), bf16),
            pltpu.VMEM((1, fine_total), jnp.int32),
            pltpu.VMEM((mid_dev, width), f32),
            pltpu.VMEM((1, mid_dev), jnp.int32),
            pltpu.VMEM((coarse_total, width), f32),
            pltpu.VMEM((1, lanes), jnp.int32),
            pltpu.SemaphoreType.DMA((7,)),
            pltpu.SemaphoreType.DMA((leaves,)),
            pltpu.SemaphoreType.DMA((lands,)),
        ],
        compiler_params=pltpu.CompilerParams(
            collective_id=0, has_side_effects=True, vmem_limit_bytes=54 * 1024 * 1024
        ),
        name="lloyd_step",
    )(
        samples,
        cell_of_row.reshape(1, row_count),
        fine_centroids,
        sharpness,
        mid_of_fine.reshape(1, fine_total),
        mid_centroids,
        coarse_of_mid.reshape(1, mid_dev),
        coarse_centroids,
    )
    return pl.pallas_call(
        put_out_kernel,
        out_shape=tuple(jax.ShapeDtypeStruct(one.shape, one.dtype) for one in results),
        in_specs=[vmem] * 4,
        out_specs=(hbm,) * 4,
        scratch_shapes=[pltpu.SemaphoreType.DMA((4,))],
        compiler_params=pltpu.CompilerParams(vmem_limit_bytes=1024 * 1024),
        name="put_out",
    )(*results)


def put_out_kernel(*refs):
    copies = [
        pltpu.make_async_copy(source, target, refs[8].at[at])
        for at, (source, target) in enumerate(zip(refs[:4], refs[4:8]))
    ]
    for copy in copies:
        copy.start()
    for copy in copies:
        copy.wait()


def solution(mesh):
    split = Mesh(
        mesh.devices.reshape(mesh.shape["group"], 4, 4, 2),
        ("group", "member_0", "member_1", "member_2"),
    )
    placed = (
        P(GROUP_MEMBER, None),
        P(GROUP_MEMBER, None),
        P(GROUP_MEMBER, None),
        P(GROUP_MEMBER),
        P(GROUP_MEMBER),
        P(GROUP_MEMBER, None),
        P(GROUP_MEMBER),
        P(),
    )
    return jax.shard_map(
        shards,
        mesh=split,
        in_specs=placed,
        out_specs=(P(GROUP_MEMBER, None), P(GROUP_MEMBER, None), P(), P(GROUP_MEMBER, None)),
        check_vma=False,
    )
```

```python
import math

import jax
import jax.numpy as jnp
from jax import lax
from jax.experimental import pallas as pl
from jax.experimental.pallas import tpu as pltpu
from jax.sharding import Mesh
from jax.sharding import PartitionSpec as P

MEMBER = ("member_0", "member_1", "member_2")
GROUP_MEMBER = ("group", "member_0", "member_1", "member_2")
RINGS = ("group", "member_0", "member_1")
CORE = "member_2"
EMPTY = 64.0
MESH_ID = pl.DeviceIdType.MESH


class Wires:
    def __init__(self, send_sem, recv_sem):
        self.send_sem, self.recv_sem = send_sem, recv_sem
        self.arrivals, self.leave = 0, []
        self.other = 1 - lax.axis_index(CORE)

    def leaving(self, like):
        self.leave.append(like)
        return len(self.leave) - 1

    def landing(self):
        self.arrivals += 1
        return self.arrivals - 1

    def copy(self, source, target, to, send_at, recv_at):
        return pltpu.make_async_remote_copy(
            src_ref=source,
            dst_ref=target,
            send_sem=self.send_sem.at[send_at],
            recv_sem=self.recv_sem.at[recv_at],
            device_id=to,
            device_id_type=MESH_ID,
        )

    def send(self, source, target, to, send_at, recv_at):
        self.copy(source, target, to, send_at, recv_at).start()

    def landed(self, like, recv_at):
        self.copy(like, like, {CORE: self.other}, 0, recv_at).wait_recv()

    def drain(self):
        for at, like in enumerate(self.leave):
            self.copy(like, like, {CORE: self.other}, at, 0).wait_send()


def greet(peers):
    for peer in peers:
        pl.semaphore_signal(
            pltpu.get_barrier_semaphore(), inc=1, device_id=peer, device_id_type=MESH_ID
        )


def greeted(peers):
    pl.semaphore_wait(pltpu.get_barrier_semaphore(), len(peers))


def ring_places(axis):
    me = lax.axis_index(axis)
    return me, lax.rem(me + 1, 4), lax.rem(me + 3, 4), lax.rem(me + 2, 4)


def ring_peers(both_cores):
    core = lax.axis_index(CORE)
    peers = [{CORE: 1 - core}]
    for axis in RINGS:
        for to in ring_places(axis)[1:]:
            peers.append({axis: to})
            if both_cores:
                peers.append({axis: to, CORE: 1 - core})
    return peers


class Exchange:
    def __init__(self, wires, refs):
        self.wires, self.refs = wires, refs
        self.core = lax.axis_index(CORE)
        self.rings = [ring_places(axis) for axis in RINGS]
        self.chunks = range(refs[0].shape[0])
        self.leave = [wires.leaving(ref.at[:, pl.ds(0, 3)]) for ref in refs[:3]]
        self.leave.append(wires.leaving(refs[2].at[:, 0, :, :, 0]))
        self.land = [[wires.landing() for _ in self.chunks] for _ in range(4)]

    def spot(self, chunk, dim, index, core_at=slice(None)):
        at = [chunk, slice(None), slice(None), slice(None), core_at]
        at[dim + 1] = index
        return tuple(at)

    def start(self, phase, chunk):
        wires, core, other = self.wires, self.core, 1 - self.core
        dim = (chunk + phase) % 3
        source, target = self.refs[phase], self.refs[phase + 1]
        axis = RINGS[dim]
        me, up, down, across = self.rings[dim]
        leave, land = self.leave[phase], self.land[phase][chunk]
        if phase < 2:
            for to in (across, up, down):
                wires.send(
                    source.at[self.spot(chunk, dim, to)],
                    target.at[self.spot(chunk, dim, me)],
                    {axis: to},
                    leave,
                    land,
                )
            own = self.spot(chunk, dim, me)
        else:
            own = self.spot(chunk, dim, me, core)
            for to in (across, up, down):
                for core_at in (0, 1):
                    wires.send(
                        source.at[self.spot(chunk, dim, to, core_at)],
                        target.at[own],
                        {axis: to, CORE: core_at},
                        leave,
                        land,
                    )
            wires.send(
                source.at[self.spot(chunk, dim, me, other)],
                target.at[own],
                {CORE: other},
                self.leave[3],
                self.land[3][chunk],
            )
        target[own] = source[own]

    def finish(self, phase, chunk):
        target = self.refs[phase + 1]
        self.wires.landed(target.at[chunk, pl.ds(0, 3)], self.land[phase][chunk])
        if phase == 2:
            self.wires.landed(target.at[chunk, 0, :, :, 0], self.land[3][chunk])

    def advance(self, phase, chunks=None):
        for chunk in self.chunks if chunks is None else chunks:
            self.finish(phase, chunk)
            if phase < 2:
                self.start(phase + 1, chunk)


class Octet:
    def __init__(self, wires):
        self.wires = wires
        self.me = lax.axis_index("member_0") * 2 + lax.axis_index(CORE)

    def start(self, source_of, targets):
        self.like = targets.at[pl.ds(0, 7)]
        leave, self.land = self.wires.leaving(self.like), self.wires.landing()
        for step in range(1, 8):
            to = lax.rem(self.me + step, 8)
            where = {"member_0": to // 2, CORE: lax.rem(to, 2)}
            self.wires.send(source_of(to), targets.at[self.me], where, leave, self.land)

    def finish(self):
        self.wires.landed(self.like, self.land)


class Ring:
    def __init__(self, wires, axis):
        self.wires, self.axis = wires, axis
        self.me, self.up, self.down, self.across = ring_places(axis)

    def order(self):
        return (self.across, self.up, self.down)

    def open(self, targets):
        self.like, self.target = targets.at[pl.ds(0, 3)], targets.at[self.me]
        self.leave, self.land = self.wires.leaving(self.like), self.wires.landing()

    def send(self, way, source):
        self.wires.send(
            source, self.target, {self.axis: self.order()[way]}, self.leave, self.land
        )

    def start(self, source_of, targets):
        self.open(targets)
        for way, to in enumerate(self.order()):
            self.send(way, source_of(to))

    def finish(self):
        self.wires.landed(self.like, self.land)


class Halves:
    def __init__(self, wires, ring, relay, near):
        self.wires, self.ring, self.relay, self.near = wires, ring, relay, near
        self.leave_relay, self.leave_near = wires.leaving(relay), wires.leaving(near)
        self.land_relay = [wires.landing() for _ in range(2)]
        self.land_near = wires.landing()

    def send_near(self, blocks, way, half):
        to = (self.ring.up, self.ring.down)[way]
        part = pl.ds(2 * half, 2)
        self.wires.send(
            blocks.at[to, part],
            self.near.at[way, part],
            {self.ring.axis: to},
            self.leave_near,
            self.land_near,
        )

    def offer(self, step, blocks):
        if step > 0:
            self.send_near(blocks, step - 1, 2 - step)
            return
        for way, to in enumerate((self.ring.up, self.ring.down)):
            self.wires.send(
                blocks.at[self.ring.across, pl.ds(2 * way, 2)],
                self.relay.at[way],
                {self.ring.axis: to},
                self.leave_relay,
                self.land_relay[way],
            )

    def pass_on(self, blocks):
        for way, to in enumerate((self.ring.up, self.ring.down)):
            self.wires.landed(self.relay.at[way], self.land_relay[way])
            for at in range(2):
                blocks[to, 2 * way + at] = (
                    blocks[to, 2 * way + at].astype(jnp.float32)
                    + self.relay[way, at].astype(jnp.float32)
                ).astype(jnp.bfloat16)
            self.send_near(blocks, way, way)

    def finish(self):
        self.wires.landed(self.near, self.land_near)


def diagonal(rows, lanes):
    return lax.broadcasted_iota(jnp.int32, (rows, lanes), 0) == lax.broadcasted_iota(
        jnp.int32, (rows, lanes), 1
    )


def as_column(row, rows):
    return jnp.sum(
        jnp.where(diagonal(rows, row.shape[1]), row, jnp.zeros_like(row)), axis=1, keepdims=True
    )


def step_kernel(
    samples_in,
    cell_in,
    fine_in,
    sharp_ref,
    mid_in,
    mids_in,
    route_in,
    coarse_in,
    fine_new_ref,
    mids_new_ref,
    coarse_new_ref,
    rec_ref,
    outgoing,
    there_a,
    there_b,
    arrived,
    rebuilt,
    back_a,
    back_b,
    returned,
    wide,
    back,
    lines,
    products,
    norms,
    shares,
    turned,
    resps,
    sums,
    chosen,
    maps,
    give,
    core_in,
    half_a,
    half_b,
    near_a,
    near_b,
    relay_a,
    relay_b,
    line_a,
    line_b,
    far_a,
    far_b,
    give_m,
    core_m,
    half_m,
    near_m,
    line_m,
    far_m,
    part_c,
    first_sum,
    second_sum,
    third_sum,
    total,
    samples_ref,
    cell_ref,
    fine_ref,
    mid_ref,
    mids_ref,
    route_ref,
    coarse_ref,
    route_wide,
    load_sem,
    send_sem,
    recv_sem,
):
    f32, bf16 = jnp.float32, jnp.bfloat16
    loads = [
        pltpu.make_async_copy(source, target, load_sem.at[at])
        for at, (source, target) in enumerate(
            (
                (cell_in, cell_ref),
                (samples_in, samples_ref),
                (route_in, route_ref),
                (fine_in, fine_ref),
                (mid_in, mid_ref),
                (mids_in, mids_ref),
                (coarse_in, coarse_ref),
            )
        )
    ]
    for load in loads:
        load.start()
    wires = Wires(send_sem, recv_sem)
    core = lax.axis_index(CORE)
    other = 1 - core
    chunks, lanes = outgoing.shape[0], outgoing.shape[-1]
    row_count, width = samples_ref.shape
    slots = chosen.shape[1]
    cells = sharp_ref.shape[0]
    fine = fine_ref.shape[0] // cells
    per_source = 2 * cells
    sources = slots // per_source
    mid_dev = mids_ref.shape[0]
    split = half_a.shape[-1]

    peers = ring_peers(True)
    greet(peers)
    loads[0].wait()
    cell_row = cell_ref[...]
    cell_column = as_column(cell_row, row_count)
    earlier = lax.broadcasted_iota(jnp.int32, (row_count, row_count), 0) < lax.broadcasted_iota(
        jnp.int32, (row_count, row_count), 1
    )
    rank = jnp.sum(
        jnp.where((cell_column == cell_row) & earlier, 1, 0), axis=0, keepdims=True
    )
    slot_row = cell_row * 2 + rank
    place = lax.broadcasted_iota(jnp.int32, (slots, row_count), 0)
    picked = jnp.where(place == slot_row, 1.0, 0.0).astype(bf16)
    used = jnp.dot(picked, jnp.ones((row_count, lanes), bf16), preferred_element_type=f32) > 0.5

    for load in loads[1:]:
        load.wait()
    route_wide[...] = jnp.zeros_like(route_wide)
    route_wide[:, pl.ds(0, mid_dev)] = route_ref[...]
    greeted(peers)
    moving = Exchange(wires, (outgoing, there_a, there_b, arrived))
    for chunk in range(0, chunks, 2):
        put = jnp.dot(
            picked, samples_ref[:, pl.ds(chunk * lanes, 2 * lanes)], preferred_element_type=f32
        )
        for at in range(2):
            line = jnp.where(used, put[:, at * lanes : (at + 1) * lanes], EMPTY)
            outgoing[chunk + at] = line.reshape(outgoing.shape[1:]).astype(bf16)
            moving.start(0, chunk + at)
    octet = Octet(wires)
    xs, zs, ys = Ring(wires, "member_0"), Ring(wires, "member_1"), Ring(wires, "group")
    maps_ring = Ring(wires, "member_1")
    octet.start(lambda to: route_wide, maps.at[zs.me])
    maps[zs.me, octet.me] = route_wide[...]
    slot_column = as_column(slot_row, row_count)
    along = lax.broadcasted_iota(jnp.int32, (row_count, slots), 1)
    chosen[...] = jnp.where(along == slot_column, 1.0, 0.0).astype(bf16)
    moving.advance(0)
    octet.finish()
    maps_ring.start(lambda to: maps.at[zs.me], maps)
    for cell in range(cells):
        here = pl.ds(cell * fine, fine)
        centres_wide = fine_ref[here, :].astype(f32)
        norms[here, :] = jnp.broadcast_to(
            jnp.sum(centres_wide * centres_wide, axis=1, keepdims=True), (fine, lanes)
        )
    moving.advance(1)
    maps_ring.finish()

    for pair in range(0, chunks, 2):
        moving.advance(2, (pair, pair + 1))
        for chunk in (pair, pair + 1):
            piece = arrived[chunk].astype(f32).reshape(slots, lanes)
            wide[chunk] = jnp.where(piece > 0.5 * EMPTY, 0.0, piece)
            if chunk == 0:
                wide[chunks] = jnp.where(piece > 0.5 * EMPTY, 0.0, 1.0)
        at = pl.ds(pair * lanes, 2 * lanes)
        for cell in range(cells):
            spots = [pl.ds(cell * 2 + most, sources, stride=per_source) for most in range(2)]
            for chunk in (pair, pair + 1) + ((chunks,) if pair == 0 else ()):
                lines[cell, :, pl.ds(chunk * lanes, lanes)] = jnp.concatenate(
                    [wide[chunk, spot, :] for spot in spots], axis=0
                ).astype(bf16)
            product = lax.dot_general(
                fine_ref[pl.ds(cell * fine, fine), at],
                lines[cell, :, at],
                (((1,), (1,)), ((), ())),
                preferred_element_type=f32,
            )
            products[cell] = product if pair == 0 else products[cell] + product

    for cell in range(cells):
        half_norms = 0.5 * norms[pl.ds(cell * fine, fine), :]
        half_norms = jnp.concatenate([half_norms, half_norms], axis=1)
        scores = (products[cell] - half_norms) * (sharp_ref[cell] / math.sqrt(width))
        exponent = jnp.exp(scores - jnp.max(scores, axis=0, keepdims=True))
        resp = exponent / jnp.sum(exponent, axis=0, keepdims=True)
        resps[cell] = resp.astype(bf16)
        turned[cell] = resp.T.astype(bf16)
    homing = Exchange(wires, (rebuilt, back_a, back_b, returned))
    for pair in range(0, chunks, 2):
        for cell in range(cells):
            row = jnp.dot(
                turned[cell],
                fine_ref[pl.ds(cell * fine, fine), pl.ds(pair * lanes, 2 * lanes)],
                preferred_element_type=f32,
            )
            for at in range(2):
                for most in range(2):
                    back[pair + at, pl.ds(cell * 2 + most, sources, stride=per_source), :] = row[
                        most * sources : (most + 1) * sources, at * lanes : (at + 1) * lanes
                    ]
        for chunk in (pair, pair + 1):
            rebuilt[chunk] = back[chunk].reshape(rebuilt.shape[1:]).astype(bf16)
            homing.start(0, chunk)

    for cell in range(cells):
        here = pl.ds(cell * fine, fine)
        weighted = jnp.dot(resps[cell], lines[cell], preferred_element_type=f32)
        sums[here, :] = weighted.astype(bf16)
        fine_new_ref[here, :] = weighted[:, :width]
        shares[here, :] = 1.0 / (weighted[:, width:] + 1.0)

    rows_of = 4 * mid_dev
    local_mid = mid_ref[...] - lax.axis_index("group") * (32 * mid_dev)
    spread = lax.broadcasted_iota(jnp.int32, (rows_of, fine_ref.shape[0]), 0)
    spread = (spread // mid_dev) * (2 * mid_dev) + spread % mid_dev

    def mid_part(x, core_at):
        wanted = local_mid - (x * 8 + core_at) * mid_dev
        picker = jnp.where(spread == wanted, 1.0, 0.0).astype(bf16)
        return jnp.dot(picker, sums[...], preferred_element_type=f32)

    def mass_row(part, z):
        tile = part[z * mid_dev : (z + 1) * mid_dev, width:]
        return jnp.sum(
            jnp.where(diagonal(mid_dev, lanes), tile, 0.0), axis=0, keepdims=True
        )

    order_x = xs.order() + (xs.me,)
    swap = [wires.landing() for _ in range(4)]
    swap_m = [wires.landing() for _ in range(4)]
    leave, leave_m = wires.leaving(give), wires.leaving(give_m)
    for way, x in enumerate(order_x):
        part = mid_part(x, other)
        for z in range(4):
            give[x, z] = part[z * mid_dev : (z + 1) * mid_dev, :width].astype(bf16)
            give_m[x, z] = mass_row(part, z)
        wires.send(give.at[x], core_in.at[x], {CORE: other}, leave, swap[way])
        wires.send(give_m.at[x], core_m.at[x], {CORE: other}, leave_m, swap_m[way])
    xs_m = Ring(wires, "member_0")
    xs_m.open(near_m)
    ring_a, ring_b = Halves(wires, xs, relay_a, near_a), Halves(wires, zs, relay_b, near_b)
    level = lax.broadcasted_iota(jnp.int32, (coarse_ref.shape[0], lanes), 0)
    coarse_part = jnp.zeros((coarse_ref.shape[0], width), f32)
    coarse_mass = jnp.zeros((coarse_ref.shape[0], lanes), f32)
    for way, x in enumerate(order_x):
        part = mid_part(x, core)
        wires.landed(core_in.at[x], swap[way])
        wires.landed(core_m.at[x], swap_m[way])
        for z in range(4):
            half = part[z * mid_dev : (z + 1) * mid_dev, :width] + core_in[x, z].astype(f32)
            half = half.astype(bf16)
            half_a[x, z] = half[:, :split]
            half_b[z, x] = half[:, split:]
            masses = mass_row(part, z) + core_m[x, z]
            half_m[x, z] = masses
            goes = level == maps[z, x * 2 + core]
            coarse_mass += jnp.where(goes, masses, 0.0)
            coarse_part += jnp.dot(
                jnp.where(goes, 1.0, 0.0).astype(bf16)[:, :mid_dev],
                half,
                preferred_element_type=f32,
            )
        if way < 3:
            ring_a.offer(way, half_a)
            xs_m.send(way, half_m.at[x])
    ring_a.pass_on(half_a)
    for way in range(3):
        ring_b.offer(way, half_b)
    coarse_mass = jnp.broadcast_to(jnp.sum(coarse_mass, axis=1, keepdims=True), coarse_mass.shape)
    for at in range(8):
        part_c[at, :, pl.ds(0, width)] = coarse_part[8 * at : 8 * at + 8].astype(bf16)
        part_c[at, :, pl.ds(width, lanes)] = coarse_mass[8 * at : 8 * at + 8].astype(bf16)
    octet.start(lambda to: part_c.at[to], first_sum)
    first_sum[octet.me] = part_c[octet.me]

    homing.advance(0, (2, 5, 0, 3))
    ring_b.pass_on(half_b)
    homing.advance(0, (1, 4))
    for cell in range(cells):
        here = pl.ds(cell * fine, fine)
        for chunk in range(chunks):
            at = pl.ds(chunk * lanes, lanes)
            fine_new_ref[here, at] = (
                fine_new_ref[here, at] + fine_ref[here, at].astype(f32)
            ) * shares[here, :]
    ring_a.finish()
    xs_m.finish()
    octet.finish()
    second_sum[ys.me] = sum(first_sum[at].astype(f32) for at in range(8))
    ys.start(lambda to: second_sum.at[ys.me], second_sum)
    for z in range(4):
        line_a[z] = (
            half_a[xs.me, z].astype(f32) + near_a[0, z].astype(f32) + near_a[1, z].astype(f32)
        ).astype(bf16)
        line_m[z] = half_m[xs.me, z] + sum(near_m[at, z] for at in xs.order())
    zs_late, zs_m, xs_late = Ring(wires, "member_1"), Ring(wires, "member_1"), Ring(wires, "member_0")

    homing.advance(1, (2, 5))
    ys.finish()
    third_sum[zs.me] = sum(second_sum[at] for at in range(4))
    zs_coarse = Ring(wires, "member_1")
    zs_coarse.start(lambda to: third_sum.at[zs.me], third_sum)
    ring_b.finish()
    for x in range(4):
        line_b[x] = (
            half_b[zs.me, x].astype(f32) + near_b[0, x].astype(f32) + near_b[1, x].astype(f32)
        ).astype(bf16)
    xs_late.start(lambda to: line_b.at[to], far_b)

    homing.advance(1, (0, 3))
    zs_late.start(lambda to: line_a.at[to], far_a)
    zs_m.start(lambda to: line_m.at[to], far_m)
    homing.advance(1, (1, 4))
    zs_coarse.finish()
    total[octet.me] = sum(third_sum[at] for at in range(4)).astype(bf16)
    octet.start(lambda to: total.at[octet.me], total)

    def reconstruct(pair):
        homing.advance(2, pair)
        found = jnp.concatenate(
            [returned[chunk].astype(f32).reshape(slots, lanes).astype(bf16) for chunk in pair],
            axis=1,
        )
        found = jnp.dot(chosen[...], found, preferred_element_type=f32).astype(bf16)
        for at, chunk in enumerate(pair):
            rec_ref[:, pl.ds(chunk * lanes, lanes)] = found[:, at * lanes : (at + 1) * lanes]

    reconstruct((2, 5))
    zs_late.finish()
    zs_m.finish()
    xs_late.finish()
    masses = line_m[zs.me] + sum(far_m[at] for at in zs.order())
    share = 1.0 / (as_column(masses, mid_dev) + 1.0)
    own_a = line_a[zs.me].astype(f32) + sum(far_a[at].astype(f32) for at in zs.order())
    own_b = line_b[xs.me].astype(f32) + sum(far_b[at].astype(f32) for at in xs.order())
    mids_new_ref[:, pl.ds(0, split)] = (own_a + mids_ref[:, pl.ds(0, split)]) * share
    mids_new_ref[:, pl.ds(split, split)] = (own_b + mids_ref[:, pl.ds(split, split)]) * share

    reconstruct((0, 3))
    reconstruct((1, 4))

    octet.finish()
    for at in range(8):
        here = pl.ds(8 * at, 8)
        share = 1.0 / (total[at, :, pl.ds(width, lanes)].astype(f32) + 1.0)
        for chunk in range(chunks):
            there = pl.ds(chunk * lanes, lanes)
            coarse_new_ref[here, there] = (
                total[at, :, there].astype(f32) + coarse_ref[here, there]
            ) * share
    wires.drain()


def shards(
    samples,
    cell_of_row,
    fine_centroids,
    sharpness,
    mid_of_fine,
    mid_centroids,
    coarse_of_mid,
    coarse_centroids,
):
    row_count, width = samples.shape
    cells = sharpness.shape[0]
    fine_total = fine_centroids.shape[0]
    fine = fine_total // cells
    mid_dev = mid_centroids.shape[0]
    coarse_total = coarse_centroids.shape[0]
    lanes = 128
    chunks = width // lanes
    slots = 128 * 2 * cells
    split = width // 2
    moved = (chunks, 4, 4, 4, 2, 2 * cells, lanes)
    eighth = (coarse_total // 8, width + lanes)
    leaves, lands = 2 * 4 + 3 + 7 + 2 + 4, 2 * 4 * chunks + 3 + 7 + 8 + 6
    f32, bf16 = jnp.float32, jnp.bfloat16
    vmem = pl.BlockSpec(memory_space=pltpu.VMEM)
    hbm = pl.BlockSpec(memory_space=pltpu.HBM)
    results = pl.pallas_call(
        step_kernel,
        out_shape=(
            pltpu.VMEM((fine_total, width), f32),
            pltpu.VMEM((mid_dev, width), f32),
            pltpu.VMEM((coarse_total, width), f32),
            pltpu.VMEM((row_count, width), bf16),
        ),
        in_specs=[hbm] * 3 + [pl.BlockSpec(memory_space=pltpu.SMEM)] + [hbm] * 4,
        out_specs=(vmem,) * 4,
        scratch_shapes=[pltpu.VMEM(moved, bf16)] * 8
        + [
            pltpu.VMEM((chunks + 1, slots, lanes), f32),
            pltpu.VMEM((chunks, slots, lanes), f32),
            pltpu.VMEM((cells, 2 * 128, width + lanes), bf16),
            pltpu.VMEM((cells, fine, 2 * 128), f32),
            pltpu.VMEM((fine_total, lanes), f32),
            pltpu.VMEM((fine_total, lanes), f32),
            pltpu.VMEM((cells, 2 * 128, fine), bf16),
            pltpu.VMEM((cells, fine, 2 * 128), bf16),
            pltpu.VMEM((fine_total, width + lanes), bf16),
            pltpu.VMEM((row_count, slots), bf16),
            pltpu.VMEM((4, 8, 1, lanes), jnp.int32),
            pltpu.VMEM((4, 4, mid_dev, width), bf16),
            pltpu.VMEM((4, 4, mid_dev, width), bf16),
        ]
        + [pltpu.VMEM((4, 4, mid_dev, split), bf16)] * 2
        + [pltpu.VMEM((2, 4, mid_dev, split), bf16)] * 2
        + [pltpu.VMEM((2, 2, mid_dev, split), bf16)] * 2
        + [pltpu.VMEM((4, mid_dev, split), bf16)] * 4
        + [pltpu.VMEM((4, 4, 1, lanes), f32)] * 4
        + [pltpu.VMEM((4, 1, lanes), f32)] * 2
        + [pltpu.VMEM((8,) + eighth, bf16)] * 2
        + [pltpu.VMEM((4,) + eighth, f32)] * 2
        + [
            pltpu.VMEM((8,) + eighth, bf16),
            pltpu.VMEM((row_count, width), bf16),
            pltpu.VMEM((1, row_count), jnp.int32),
            pltpu.VMEM((fine_total, width), bf16),
            pltpu.VMEM((1, fine_total), jnp.int32),
            pltpu.VMEM((mid_dev, width), f32),
            pltpu.VMEM((1, mid_dev), jnp.int32),
            pltpu.VMEM((coarse_total, width), f32),
            pltpu.VMEM((1, lanes), jnp.int32),
            pltpu.SemaphoreType.DMA((7,)),
            pltpu.SemaphoreType.DMA((leaves,)),
            pltpu.SemaphoreType.DMA((lands,)),
        ],
        compiler_params=pltpu.CompilerParams(
            collective_id=0, has_side_effects=True, vmem_limit_bytes=54 * 1024 * 1024
        ),
        name="lloyd_step",
    )(
        samples,
        cell_of_row.reshape(1, row_count),
        fine_centroids,
        sharpness,
        mid_of_fine.reshape(1, fine_total),
        mid_centroids,
        coarse_of_mid.reshape(1, mid_dev),
        coarse_centroids,
    )
    return pl.pallas_call(
        put_out_kernel,
        out_shape=tuple(jax.ShapeDtypeStruct(one.shape, one.dtype) for one in results),
        in_specs=[vmem] * 4,
        out_specs=(hbm,) * 4,
        scratch_shapes=[pltpu.SemaphoreType.DMA((4,))],
        compiler_params=pltpu.CompilerParams(vmem_limit_bytes=1024 * 1024),
        name="put_out",
    )(*results)


def put_out_kernel(*refs):
    copies = [
        pltpu.make_async_copy(source, target, refs[8].at[at])
        for at, (source, target) in enumerate(zip(refs[:4], refs[4:8]))
    ]
    for copy in copies:
        copy.start()
    for copy in copies:
        copy.wait()


def solution(mesh):
    split = Mesh(
        mesh.devices.reshape(mesh.shape["group"], 4, 4, 2),
        ("group", "member_0", "member_1", "member_2"),
    )
    placed = (
        P(GROUP_MEMBER, None),
        P(GROUP_MEMBER, None),
        P(GROUP_MEMBER, None),
        P(GROUP_MEMBER),
        P(GROUP_MEMBER),
        P(GROUP_MEMBER, None),
        P(GROUP_MEMBER),
        P(),
    )
    return jax.shard_map(
        shards,
        mesh=split,
        in_specs=placed,
        out_specs=(P(GROUP_MEMBER, None), P(GROUP_MEMBER, None), P(), P(GROUP_MEMBER, None)),
        check_vma=False,
    )
```
